32 devices in a mesh: dp: 32 (over z, y, x, core).
Axes of the slice: x: 2, y: 2, z: 4, core: 2. Of those that a mesh axis runs over, the one named last changes fastest.
Arguments:
- params: float32 [4063232], P('dp'), may hold values from -6 to 6
- first_moment: float32 [4063232], P('dp'), may hold values from -2 to 2
- second_moment: float32 [4063232], P('dp'), may hold values from 0.01 to 1
- grads: bfloat16 [4063232], P('dp'), may hold values from -6 to 6
- old_bounds: int32 [33], replicated, may hold values from 0 to 3932160, as said below
- new_bounds: int32 [33], replicated, may hold values from 0 to 3932160, as said below
- seg_start: int32 [64], replicated, may hold values from 0 to 3932096, as said below
Outputs:
- new_params: float32 [4063232], P('dp')
- new_first: float32 [4063232], P('dp')
- new_second: float32 [4063232], P('dp')
The draws below stay inside these ranges and needn't reach their ends.
Inputs may be any that keep to these rules, and one draw needn't show every extreme that they name: `old_bounds`: starts at 0 and ends at 3932160; every shard holds between 118784 and 126976 elements, exactly 126976 in some shard. `new_bounds`: starts at 0 and ends at 3932160; every shard holds between 118784 and 126976 elements, exactly 126976 in some shard; each entry differs from the same entry of old_bounds by at most 4096, by exactly 4096 somewhere. `seg_start`: strictly rising, the first is 0, all are multiples of 64.
All inputs are finite; a program needn't handle non-finite values.
Results may differ from the reference program's by a relative error of at most 0.0003.
Values sent between devices are 32-bit elements; how exact they have to be, the bound alone decides.
A program may use at most 64 MiB of HBM per device.

```python
import math
import jax
import jax.numpy as jnp

BASE = 122880
MARGIN = 4096
SEGS = 64
CAP = 126976
TOTAL = 3932160
N_DP = 32


def bounds_pair(key):
    half = MARGIN // 2
    first = jax.random.randint(jax.random.fold_in(key, 11), (N_DP + 1,), -half, half + 1)
    second = jax.random.randint(jax.random.fold_in(key, 12), (N_DP + 1,), -half, half + 1)
    where_at = jax.random.randint(jax.random.fold_in(key, 13), (), 1, N_DP - 2)
    index = jnp.arange(N_DP + 1, dtype=jnp.int32)
    first = jnp.where(index == where_at, -half, first)
    first = jnp.where(index == where_at + 1, half, first)
    second = jnp.where(index == where_at + 1, -half, second)
    second = jnp.where(index == where_at + 2, half, second)
    edges = (index == 0) | (index == N_DP)
    first = jnp.where(edges, 0, first)
    second = jnp.where(edges, 0, second)
    nominal = index * BASE
    return ((nominal + first).astype(jnp.int32), (nominal + second).astype(jnp.int32))


def draw_old_bounds(key, part):
    return bounds_pair(key)[0]


def draw_new_bounds(key, part):
    return bounds_pair(key)[1]


def draw_seg_start(key, part):
    picks = jax.random.permutation(jax.random.fold_in(key, 21), TOTAL // 64 - 1)[:SEGS - 1] + 1
    picks = jnp.sort(picks.astype(jnp.int32))
    return jnp.concatenate([jnp.zeros((1,), jnp.int32), picks * 64]).astype(jnp.int32)


def level_of(rng, dims, cuts, least, largest):
    loudness = 1.0
    for dim, blocks in cuts:
        heights = jax.random.uniform(jax.random.fold_in(jax.random.fold_in(rng, 6), dim), (blocks,), jnp.float32, least / len(cuts), largest / len(cuts))
        loudness = loudness * jnp.repeat(jnp.exp(heights), dims[dim] // blocks).reshape((-1,) + (1,) * (len(dims) - 1 - dim))
    return loudness


def normal_values(key, extent, spread, bound, pieces=(), kind=jnp.bfloat16):
    level = level_of(key, extent, pieces, -0.22, 0.18) if pieces else 1.0
    result = jax.random.normal(key, extent, jnp.float32) * spread * level
    return jnp.minimum(jnp.maximum(result, -bound), bound).astype(kind)


def setup_inputs(seed: int = 0) -> dict:
    streams_of = jax.random.split(jax.random.key(seed), 8)
    params = normal_values(streams_of[0], (N_DP * CAP,), 1.0, 6.0, ((0, 32),), jnp.float32)
    first_moment = normal_values(streams_of[1], (N_DP * CAP,), 0.3, 2.0, ((0, 32),), jnp.float32)
    second_moment = jnp.clip(jnp.exp(math.log(1.0) - 4.6051702 * jax.random.uniform(streams_of[2], (N_DP * CAP,), jnp.float32) ** level_of(streams_of[2], (N_DP * CAP,), ((0, 32),), -0.2, 0.2)), 0.01, 1.0)
    grads = normal_values(streams_of[3], (N_DP * CAP,), 1.0, 6.0, ((0, 32),))
    old_bounds = draw_old_bounds(jax.random.fold_in(streams_of[7], 71), 0)
    new_bounds = draw_new_bounds(jax.random.fold_in(streams_of[7], 71), 0)
    seg_start = draw_seg_start(jax.random.fold_in(streams_of[7], 71), 0)
    return {"params": params, "first_moment": first_moment, "second_moment": second_moment, "grads": grads, "old_bounds": old_bounds, "new_bounds": new_bounds, "seg_start": seg_start}


BETA_ONE = 0.9
BETA_TWO = 0.999
CORR_ONE = 1.0 - 0.9 ** 10
CORR_TWO = 1.0 - 0.999 ** 10
DECAY = 0.01
LEARN = 0.1
EPSILON = 1e-06

def reference(params, first_moment, second_moment, grads, old_bounds, new_bounds, seg_start):
    count = N_DP
    cap = BASE + MARGIN
    total = BASE * N_DP
    position = jnp.arange(total, dtype=jnp.int32)
    owner = (jnp.searchsorted(old_bounds, position, side='right') - 1).astype(jnp.int32)
    owner = jnp.clip(owner, 0, count - 1).astype(jnp.int32)
    source = (owner * cap + (position - old_bounds[owner])).astype(jnp.int32)
    weight = params[source]
    moment = first_moment[source]
    second = second_moment[source]
    gradient = grads[source].astype(jnp.float32)
    moment_new = BETA_ONE * moment + (1.0 - BETA_ONE) * gradient
    second_new = BETA_TWO * second + (1.0 - BETA_TWO) * gradient * gradient
    update = moment_new / CORR_ONE / (jnp.sqrt(second_new / CORR_TWO) + EPSILON) + DECAY * weight
    segment = (jnp.searchsorted(seg_start, position, side='right') - 1).astype(jnp.int32)
    weight_sq = jax.ops.segment_sum(weight * weight, segment, num_segments=SEGS)
    update_sq = jax.ops.segment_sum(update * update, segment, num_segments=SEGS)
    ratio = jnp.sqrt(weight_sq) / (jnp.sqrt(update_sq) + EPSILON)
    weight_new = weight - LEARN * ratio[segment] * update
    slot_index = jnp.arange(count * cap, dtype=jnp.int32)
    device = (slot_index // cap).astype(jnp.int32)
    within = (slot_index % cap).astype(jnp.int32)
    valid = within < new_bounds[device + 1] - new_bounds[device]
    target = jnp.clip(new_bounds[device] + within, 0, total - 1).astype(jnp.int32)
    zero = jnp.float32(0.0)
    return (jnp.where(valid, weight_new[target], zero), jnp.where(valid, moment_new[target], zero), jnp.where(valid, second_new[target], zero))
```

```python
import functools

import jax
import jax.numpy as jnp
from jax import lax
from jax.experimental import pallas as pl
from jax.experimental.pallas import tpu as pltpu
from jax.sharding import PartitionSpec as P

MARGIN = 4096
LANES = 128
BLOCK = MARGIN // LANES
HALF = 64
HALF_BITS = 6
LANE_BITS = 7
PAD = BLOCK + 8
EDGE = 2 * PAD + BLOCK


BETA_ONE = 0.9
BETA_TWO = 0.999
CORR_ONE = 1.0 - 0.9**10
CORR_TWO = 1.0 - 0.999**10
DECAY = 0.01
LEARN = 0.1
EPSILON = 1e-06

MESH = pl.DeviceIdType.MESH
VMEM_LIMIT = 16 * 1024 * 1024


def lane_ids(rows=BLOCK):
    return lax.broadcasted_iota(jnp.int32, (rows, LANES), 1)


def flat_ids():
    return lax.broadcasted_iota(jnp.int32, (BLOCK, LANES), 0) * LANES + lane_ids()


def moved(first, second, lanes):
    picked = jnp.where(lane_ids() >= lanes, first, second)
    return pltpu.roll(picked, (LANES - lanes) & (LANES - 1), 1)


def fetched(tables, refs, sems):
    copies = [pltpu.make_async_copy(t, r, sems.at[i]) for i, (t, r) in enumerate(zip(tables, refs))]
    for copy in copies:
        copy.start()
    return copies


def step_kernel(
    axis, n, old_hbm, new_hbm, seg_hbm, w_hbm, m_hbm, v_hbm, g_hbm, placed, sums, chosen,
    state, m_buf, v_buf, g_buf, squares, member, begins, ends, part, tail, head, left_rim, right_rim,
    before, after, slots, old_ref, new_ref, seg_ref, sems, table_sems, send, receive, rim_send, rim_receive,
):
    rows = m_buf.shape[0]
    blocks = rows // BLOCK
    segs = seg_ref.shape[0]
    me = lax.axis_index(axis)
    right = lax.rem(me + 1, n)
    left = lax.rem(me + n - 1, n)
    tables = fetched((old_hbm, new_hbm, seg_hbm), (old_ref, new_ref, seg_ref), table_sems)
    step_blocks = -(-blocks // sems.shape[1])
    chunks = [(b, min(b + step_blocks, blocks)) for b in range(0, blocks, step_blocks)]
    copies = []
    for c, (b0, b1) in enumerate(chunks):
        window = pl.ds(b0 * BLOCK, (b1 - b0) * BLOCK)
        inside = state.at[0, pl.ds(PAD + b0 * BLOCK, (b1 - b0) * BLOCK)]
        group = [
            pltpu.make_async_copy(w_hbm.at[window], inside, sems.at[0, c]),
            pltpu.make_async_copy(m_hbm.at[window], m_buf.at[window], sems.at[1, c]),
            pltpu.make_async_copy(v_hbm.at[window], v_buf.at[window], sems.at[2, c]),
            pltpu.make_async_copy(g_hbm.at[window], g_buf.at[window], sems.at[3, c]),
        ]
        for copy in group:
            copy.start()
        copies.append(group)

    barrier = pltpu.get_barrier_semaphore()

    def greet(k, carry):
        pl.semaphore_signal(barrier, inc=1, device_id=(lax.rem(me + k, n),), device_id_type=MESH)
        return carry

    lax.fori_loop(1, n, greet, 0)

    for copy in tables:
        copy.wait()
    low = old_ref[me]
    count = old_ref[me + 1] - low
    new_low = new_ref[me]
    new_count = new_ref[me + 1] - new_low
    shift = new_low - low
    phase = (-low) & (HALF - 1)

    def bound_all(origin, offset):
        def bound(s, carry):
            value = (seg_ref[s] - origin - offset) >> HALF_BITS
            begins[pl.ds(s, 1), :] = jnp.full((1, LANES), value, jnp.int32)
            following = (seg_ref[jnp.minimum(s + 1, segs - 1)] - origin - offset) >> HALF_BITS
            following = jnp.where(s + 1 < segs, following, 4 * rows)
            ends[pl.ds(s, 1), :] = jnp.full((1, LANES), following, jnp.int32)
            return carry

        lax.fori_loop(0, segs, bound, 0, unroll=8)

    bound_all(low, phase)
    padded = member.shape[1]
    spot = lane_ids(segs)
    first_half = begins[...]
    past_half = ends[...]
    for group in range(3):
        for tile in range(padded // LANES):
            half = 2 * (spot + tile * LANES) - 1 + group
            mask = (half >= first_half) & (half < past_half)
            member[group * segs : (group + 1) * segs, tile * LANES : (tile + 1) * LANES] = jnp.where(
                mask, 1.0, 0.0
            ).astype(jnp.bfloat16)
    squares[rows:padded, :] = jnp.zeros((padded - rows, 4 * LANES), jnp.bfloat16)

    flat = flat_ids()

    def advance(b, carry):
        here = pl.multiple_of(b * BLOCK, BLOCK)
        there = pl.multiple_of(b * BLOCK + PAD, 8)
        gradient = g_buf[pl.ds(here, BLOCK), :].astype(jnp.float32)
        weight = state[0, pl.ds(there, BLOCK), :]
        moment = BETA_ONE * m_buf[pl.ds(here, BLOCK), :] + (1.0 - BETA_ONE) * gradient
        second = BETA_TWO * v_buf[pl.ds(here, BLOCK), :] + (1.0 - BETA_TWO) * gradient * gradient
        scaled = moment * (1.0 / CORR_ONE)
        update = scaled / (jnp.sqrt(second * (1.0 / CORR_TWO)) + EPSILON) + DECAY * weight
        state[1, pl.ds(there, BLOCK), :] = update
        state[2, pl.ds(there, BLOCK), :] = moment
        state[3, pl.ds(there, BLOCK), :] = second
        live = flat + b * MARGIN < count
        for i, value in enumerate((weight, update)):
            square = jnp.where(live, value * value, 0.0)
            coarse = square.astype(jnp.bfloat16)
            fine = (square - coarse.astype(jnp.float32)).astype(jnp.bfloat16)
            squares[pl.ds(here, BLOCK), i * LANES : (i + 1) * LANES] = coarse
            squares[pl.ds(here, BLOCK), (i + 2) * LANES : (i + 3) * LANES] = fine
        return carry

    for (b0, b1), group in zip(chunks, copies):
        for copy in group:
            copy.wait()
        lax.fori_loop(b0, b1, advance, 0, unroll=2)

    start = count - MARGIN
    start_row = start >> LANE_BITS
    start_lane = start & (LANES - 1)
    for a in range(4):
        head[a] = state[a, PAD : PAD + BLOCK, :]
        tail[a] = moved(
            state[a, pl.ds(PAD + start_row, BLOCK), :],
            state[a, pl.ds(PAD + start_row + 1, BLOCK), :],
            start_lane,
        )

    product = jnp.dot(member[...], squares[...], preferred_element_type=jnp.float32)
    product = product[:, : 2 * LANES] + product[:, 2 * LANES :]
    line = lax.broadcasted_iota(jnp.int32, (segs, LANES), 0)
    row = jnp.zeros((segs, LANES), jnp.float32)
    for i in range(2):
        columns = slice(i * LANES, (i + 1) * LANES)
        mixed = jnp.where(
            spot < phase,
            product[0:segs, columns],
            jnp.where(
                spot < phase + HALF, product[segs : 2 * segs, columns], product[2 * segs : 3 * segs, columns]
            ),
        )
        row = jnp.where(spot == line + i * segs, jnp.sum(mixed, axis=1, keepdims=True), row)
    part[...] = jnp.sum(row, axis=0, keepdims=True)
    pl.semaphore_wait(barrier, n - 1)

    def tell(k):
        return pltpu.make_async_remote_copy(
            src_ref=part,
            dst_ref=slots.at[me],
            send_sem=send,
            recv_sem=receive,
            device_id=(lax.rem(me + k, n),),
            device_id_type=MESH,
        )

    onward = pltpu.make_async_remote_copy(
        src_ref=tail,
        dst_ref=left_rim,
        send_sem=rim_send.at[0],
        recv_sem=rim_receive.at[0],
        device_id=(right,),
        device_id_type=MESH,
    )
    back = pltpu.make_async_remote_copy(
        src_ref=head,
        dst_ref=right_rim,
        send_sem=rim_send.at[1],
        recv_sem=rim_receive.at[1],
        device_id=(left,),
        device_id_type=MESH,
    )

    for k in range(1, n):
        tell(k).start()
    pltpu.make_async_copy(part, slots.at[me], receive).start()

    @pl.when(me < n - 1)
    def send_tail():
        onward.start()

    @pl.when(me > 0)
    def send_head():
        back.start()

    top = shift >> LANE_BITS
    lanes = shift & (LANES - 1)

    def own(a, b):
        there = b * BLOCK + PAD + top
        return moved(state[a, pl.ds(there, BLOCK), :], state[a, pl.ds(there + 1, BLOCK), :], lanes)

    def inner(b, carry):
        here = pl.multiple_of(b * BLOCK, BLOCK)
        for a in range(4):
            placed[a, pl.ds(here, BLOCK), :] = own(a, b)
        return carry

    lax.fori_loop(1, blocks - 3, inner, 0, unroll=3)
    for a in range(4):
        before[a, BLOCK:EDGE, :] = state[a, PAD : PAD + EDGE - BLOCK, :]

    @pl.when(me < n - 1)
    def end_right():
        onward.wait_send()
        back.wait_recv()

    @pl.when(me > 0)
    def end_left():
        back.wait_send()
        onward.wait_recv()

    for a in range(4):
        before[a, 0:BLOCK, :] = left_rim[a]
        after[a, PAD : PAD + BLOCK, :] = right_rim[a]
    for a in range(4):
        placed[a, 0:BLOCK, :] = moved(
            before[a, pl.ds(BLOCK + top, BLOCK), :], before[a, pl.ds(BLOCK + top + 1, BLOCK), :], lanes
        )

    for b in range(blocks - 3, blocks):
        offset = b * MARGIN + shift - count
        near = jnp.clip(offset >> LANE_BITS, -PAD, PAD - 7) + PAD
        side = offset & (LANES - 1)
        index = flat + b * MARGIN
        beyond = index + shift >= count
        live = index < new_count
        for a in range(4):
            rim = moved(after[a, pl.ds(near, BLOCK), :], after[a, pl.ds(near + 1, BLOCK), :], side)
            value = jnp.where(beyond, rim, own(a, b))
            placed[a, b * BLOCK : (b + 1) * BLOCK, :] = jnp.where(live, value, 0.0)

    new_phase = (-new_low) & (HALF - 1)
    bound_all(new_low, new_phase)
    on_lane = (spot & (segs - 1)) == line
    lows = jnp.sum(jnp.where(on_lane, begins[...], 0), axis=0, keepdims=True)
    highs = jnp.sum(jnp.where(on_lane, ends[...], 0), axis=0, keepdims=True)
    block_row = lax.broadcasted_iota(jnp.int32, (BLOCK, LANES), 0)
    lane_group = lane_ids() >> HALF_BITS

    def choose(b, carry):
        here = pl.multiple_of(b * BLOCK, BLOCK)
        for tile in range(2):
            half = 2 * (block_row + b * BLOCK) - 1 + 2 * tile + lane_group
            mask = (half >= lows) & (half < highs)
            chosen[pl.ds(here, BLOCK), tile * LANES : (tile + 1) * LANES] = jnp.where(mask, 1.0, 0.0).astype(
                jnp.bfloat16
            )
        return carry

    lax.fori_loop(0, blocks, choose, 0, unroll=2)
    sums[1:2, :] = jnp.full((1, LANES), new_phase, jnp.int32).astype(jnp.float32)

    pltpu.make_async_copy(slots, slots, receive).wait()
    sums[0:1, :] = jnp.sum(slots[...], axis=0)
    others = slots.at[pl.ds(0, n - 1)]
    pltpu.make_async_copy(others, others, send).wait()


def apply_kernel(segs, placed, sums, chosen, w_out, m_out, v_out, w_buf, sems):
    m_copy = pltpu.make_async_copy(placed.at[2], m_out, sems.at[0])
    v_copy = pltpu.make_async_copy(placed.at[3], v_out, sems.at[1])
    m_copy.start()
    v_copy.start()
    rows = w_buf.shape[0]
    total = sums[0:1, :]
    phase = sums[1:2, :]
    other = pltpu.roll(total, LANES - segs, 1)
    rate = LEARN * (jnp.sqrt(total) / (jnp.sqrt(other) + EPSILON))
    spot = lane_ids(segs)
    line = lax.broadcasted_iota(jnp.int32, (segs, LANES), 0)
    column = jnp.sum(jnp.where(spot == line, rate, 0.0), axis=1, keepdims=True)
    place = spot.astype(jnp.float32)
    early = place < phase
    late = place >= phase + HALF
    nothing = jnp.zeros((segs, LANES), jnp.float32)
    rates = jnp.concatenate(
        [
            jnp.where(early, column, 0.0),
            jnp.where(early | late, 0.0, column),
            jnp.where(late, column, 0.0),
            nothing,
        ],
        axis=0,
    )
    coarse = rates.astype(jnp.bfloat16)
    fine = (rates - coarse.astype(jnp.float32)).astype(jnp.bfloat16)
    table = jnp.concatenate([coarse, fine], axis=1)
    step = 256
    copies = []
    for c, r0 in enumerate(range(0, rows, step)):
        size = min(step, rows - r0)
        product = jnp.dot(chosen[r0 : r0 + size, :], table, preferred_element_type=jnp.float32)
        factor = product[:, :LANES] + product[:, LANES:]
        w_buf[r0 : r0 + size, :] = placed[0, r0 : r0 + size, :] - factor * placed[1, r0 : r0 + size, :]
        window = pl.ds(r0, size)
        copy = pltpu.make_async_copy(w_buf.at[window], w_out.at[window], sems.at[2 + c])
        copy.start()
        copies.append(copy)
    for copy in (m_copy, v_copy, *copies):
        copy.wait()


def spec(space):
    return pl.BlockSpec(memory_space=space)


def shards(axis, n, params, first_moment, second_moment, grads, old_bounds, new_bounds, seg_start):
    cap = params.shape[0]
    rows = cap // LANES
    f32 = jnp.float32
    flat = [x.reshape(rows, LANES) for x in (params, first_moment, second_moment, grads)]
    old_bounds, new_bounds, seg_start, *flat = (
        pltpu.with_memory_space_constraint(x, pltpu.HBM) for x in (old_bounds, new_bounds, seg_start, *flat)
    )
    segs = seg_start.shape[0]
    padded = -(-rows // 256) * 256
    vmem, hbm = spec(pltpu.VMEM), spec(pltpu.HBM)
    bounds = pltpu.SMEM(old_bounds.shape, jnp.int32)
    starts = pltpu.SMEM(seg_start.shape, jnp.int32)
    rim = pltpu.VMEM((4, BLOCK, LANES), f32)
    dma = pltpu.SemaphoreType.DMA
    placed, sums, chosen = pl.pallas_call(
        functools.partial(step_kernel, axis, n),
        name="step",
        out_shape=(
            jax.ShapeDtypeStruct((4, rows, LANES), f32),
            jax.ShapeDtypeStruct((2, LANES), f32),
            jax.ShapeDtypeStruct((rows, 2 * LANES), jnp.bfloat16),
        ),
        in_specs=[hbm] * 7,
        out_specs=(vmem,) * 3,
        scratch_shapes=[
            pltpu.VMEM((4, rows + 2 * PAD, LANES), f32),
            pltpu.VMEM((rows, LANES), f32),
            pltpu.VMEM((rows, LANES), f32),
            pltpu.VMEM((rows, LANES), grads.dtype),
            pltpu.VMEM((padded, 4 * LANES), jnp.bfloat16),
            pltpu.VMEM((3 * segs, padded), jnp.bfloat16),
            pltpu.VMEM((segs, LANES), jnp.int32),
            pltpu.VMEM((segs, LANES), jnp.int32),
            pltpu.VMEM((1, LANES), f32),
            rim,
            rim,
            rim,
            rim,
            pltpu.VMEM((4, EDGE, LANES), f32),
            pltpu.VMEM((4, EDGE, LANES), f32),
            pltpu.VMEM((n, 1, LANES), f32),
            bounds,
            bounds,
            starts,
            dma((4, 2)),
            dma((3,)),
            dma,
            dma,
            dma((2,)),
            dma((2,)),
        ],
        compiler_params=pltpu.CompilerParams(
            collective_id=0, has_side_effects=True, vmem_limit_bytes=VMEM_LIMIT
        ),
    )(old_bounds, new_bounds, seg_start, *flat)
    whole = jax.ShapeDtypeStruct((rows, LANES), f32)
    outs = pl.pallas_call(
        functools.partial(apply_kernel, segs),
        name="apply",
        out_shape=(whole,) * 3,
        in_specs=[vmem] * 3,
        out_specs=(hbm,) * 3,
        scratch_shapes=[pltpu.VMEM((rows, LANES), f32), dma((2 + -(-rows // 256),))],
        compiler_params=pltpu.CompilerParams(vmem_limit_bytes=VMEM_LIMIT),
    )(placed, sums, chosen)
    return tuple(x.reshape(cap) for x in outs)


def solution(mesh):
    (axis,) = mesh.axis_names
    n = mesh.shape[axis]
    placed = (P(axis), P(axis), P(axis), P(axis), P(), P(), P())
    return jax.shard_map(
        functools.partial(shards, axis, n),
        mesh=mesh,
        in_specs=placed,
        out_specs=(P(axis), P(axis), P(axis)),
        check_vma=False,
    )
```

```python
import functools

import jax
import jax.numpy as jnp
from jax import lax
from jax.experimental import pallas as pl
from jax.experimental.pallas import tpu as pltpu
from jax.sharding import PartitionSpec as P

MARGIN = 4096
LANES = 128
BLOCK = MARGIN // LANES
HALF = 64
HALF_BITS = 6
LANE_BITS = 7
PAD = BLOCK + 8
EDGE = 2 * PAD + BLOCK
TILE = 256


BETA_ONE = 0.9
BETA_TWO = 0.999
CORR_ONE = 1.0 - 0.9**10
CORR_TWO = 1.0 - 0.999**10
DECAY = 0.01
LEARN = 0.1
EPSILON = 1e-06

MESH = pl.DeviceIdType.MESH
VMEM_LIMIT = 16 * 1024 * 1024


def lane_ids(rows=BLOCK):
    return lax.broadcasted_iota(jnp.int32, (rows, LANES), 1)


def flat_ids():
    return lax.broadcasted_iota(jnp.int32, (BLOCK, LANES), 0) * LANES + lane_ids()


def moved(first, second, lanes):
    picked = jnp.where(lane_ids() >= lanes, first, second)
    return pltpu.roll(picked, (LANES - lanes) & (LANES - 1), 1)


def fetched(tables, refs, sems):
    copies = [pltpu.make_async_copy(t, r, sems.at[i]) for i, (t, r) in enumerate(zip(tables, refs))]
    for copy in copies:
        copy.start()
    return copies


def step_kernel(
    axis, n, old_hbm, new_hbm, seg_hbm, w_hbm, m_hbm, v_hbm, g_hbm, placed, sums, chosen,
    state, m_buf, v_buf, g_buf, member, part, tail, head, left_rim, right_rim,
    before, after, slots, old_ref, new_ref, seg_ref, sems, table_sems, send, receive, rim_send, rim_receive,
):
    rows = m_buf.shape[0]
    blocks = rows // BLOCK
    segs = seg_ref.shape[1]
    me = lax.axis_index(axis)
    right = lax.rem(me + 1, n)
    left = lax.rem(me + n - 1, n)
    tables = fetched((old_hbm, new_hbm, seg_hbm), (old_ref, new_ref, seg_ref), table_sems)
    middle = -(-rows // (2 * TILE)) * TILE
    halves = []
    for c, (r0, r1) in enumerate(((0, middle), (middle, rows))):
        window = pl.ds(r0, r1 - r0)
        group = [
            pltpu.make_async_copy(g_hbm.at[window], g_buf.at[window], sems.at[3, c]),
            pltpu.make_async_copy(m_hbm.at[window], m_buf.at[window], sems.at[1, c]),
            pltpu.make_async_copy(v_hbm.at[window], v_buf.at[window], sems.at[2, c]),
            pltpu.make_async_copy(w_hbm.at[window], state.at[0, pl.ds(PAD + r0, r1 - r0)], sems.at[0, c]),
        ]
        for copy in group:
            copy.start()
        halves.append(group)

    barrier = pltpu.get_barrier_semaphore()

    def greet(k, carry):
        pl.semaphore_signal(barrier, inc=1, device_id=(lax.rem(me + k, n),), device_id_type=MESH)
        return carry

    lax.fori_loop(1, n, greet, 0)

    for copy in tables:
        copy.wait()
    low = old_ref[me]
    count = old_ref[me + 1] - low
    new_low = new_ref[me]
    new_count = new_ref[me + 1] - new_low
    shift = new_low - low
    phase = (-low) & (HALF - 1)
    spot = lane_ids(segs)
    line = lax.broadcasted_iota(jnp.int32, (segs, LANES), 0)
    square_line = lax.broadcasted_iota(jnp.int32, (segs, segs), 0)
    square_spot = lax.broadcasted_iota(jnp.int32, (segs, segs), 1)
    starts = (seg_ref[...] >> HALF_BITS).astype(jnp.float32)
    first = jnp.sum(jnp.where(square_spot == square_line, starts, 0.0), axis=1, keepdims=True)
    past = jnp.sum(jnp.where(square_spot == square_line + 1, starts, 0.0), axis=1, keepdims=True)
    past = jnp.where(square_line[:, :1] == segs - 1, 4.0 * n * rows, past)
    first = jnp.broadcast_to(first.astype(jnp.int32), (segs, LANES))
    past = jnp.broadcast_to(past.astype(jnp.int32), (segs, LANES))
    base = (low + phase) >> HALF_BITS
    first_half = first - base
    past_half = past - base
    padded = member.shape[1]
    for group in range(3):
        for tile in range(padded // LANES):
            half = 2 * (spot + tile * LANES) - 1 + group
            mask = (half >= first_half) & (half < past_half)
            member[group * segs : (group + 1) * segs, tile * LANES : (tile + 1) * LANES] = jnp.where(
                mask, 1.0, 0.0
            ).astype(jnp.bfloat16)

    flat = flat_ids()

    def advance(r0):
        here = slice(r0, r0 + BLOCK)
        there = slice(r0 + PAD, r0 + PAD + BLOCK)
        gradient = g_buf[here, :].astype(jnp.float32)
        weight = state[0, there, :]
        moment = BETA_ONE * m_buf[here, :] + (1.0 - BETA_ONE) * gradient
        second = BETA_TWO * v_buf[here, :] + ((1.0 - BETA_TWO) * gradient) * gradient
        spread = second * (CORR_ONE * CORR_ONE / CORR_TWO)
        update = moment / (spread * lax.rsqrt(spread) + CORR_ONE * EPSILON) + DECAY * weight
        state[1, there, :] = update
        state[2, there, :] = moment
        state[3, there, :] = second
        return weight, update

    for copy in halves[0]:
        copy.wait()
    for r0 in range(0, middle, BLOCK):
        advance(r0)
    for copy in halves[1]:
        copy.wait()
    product = None
    for t0 in range(0, rows, TILE):
        t1 = min(t0 + TILE, rows)
        pieces = [[], [], [], []]
        for r0 in range(t0, t1, BLOCK):
            if r0 < middle:
                values = [state[a, r0 + PAD : r0 + PAD + BLOCK, :] for a in range(2)]
            else:
                values = advance(r0)
            for i, value in enumerate(values):
                square = value * value
                if r0 + 2 * BLOCK >= rows:
                    square = jnp.where(flat + r0 * LANES < count, square, 0.0)
                coarse = square.astype(jnp.bfloat16)
                pieces[i].append(coarse)
                pieces[i + 2].append((square - coarse.astype(jnp.float32)).astype(jnp.bfloat16))
        squares = jnp.concatenate([jnp.concatenate(p, axis=0) for p in pieces], axis=1)
        partial = jnp.dot(member[:, t0:t1], squares, preferred_element_type=jnp.float32)
        product = partial if product is None else product + partial
    product = product[:, : 2 * LANES] + product[:, 2 * LANES :]
    row = jnp.zeros((segs, LANES), jnp.float32)
    for i in range(2):
        columns = slice(i * LANES, (i + 1) * LANES)
        mixed = jnp.where(
            spot < phase,
            product[0:segs, columns],
            jnp.where(
                spot < phase + HALF, product[segs : 2 * segs, columns], product[2 * segs : 3 * segs, columns]
            ),
        )
        row = jnp.where(spot == line + i * segs, jnp.sum(mixed, axis=1, keepdims=True), row)
    part[...] = jnp.sum(row, axis=0, keepdims=True)
    pl.semaphore_wait(barrier, n - 1)

    def tell(k):
        return pltpu.make_async_remote_copy(
            src_ref=part,
            dst_ref=slots.at[me],
            send_sem=send,
            recv_sem=receive,
            device_id=(lax.rem(me + k, n),),
            device_id_type=MESH,
        )

    onward = pltpu.make_async_remote_copy(
        src_ref=tail,
        dst_ref=left_rim,
        send_sem=rim_send.at[0],
        recv_sem=rim_receive.at[0],
        device_id=(right,),
        device_id_type=MESH,
    )
    back = pltpu.make_async_remote_copy(
        src_ref=head,
        dst_ref=right_rim,
        send_sem=rim_send.at[1],
        recv_sem=rim_receive.at[1],
        device_id=(left,),
        device_id_type=MESH,
    )

    for k in range(1, n):
        tell(k).start()
    pltpu.make_async_copy(part, slots.at[me], receive).start()

    start = count - MARGIN
    start_row = start >> LANE_BITS
    start_lane = start & (LANES - 1)
    for a in range(4):
        head[a] = state[a, PAD : PAD + BLOCK, :]
        tail[a] = moved(
            state[a, pl.ds(PAD + start_row, BLOCK), :],
            state[a, pl.ds(PAD + start_row + 1, BLOCK), :],
            start_lane,
        )

    @pl.when(me < n - 1)
    def send_tail():
        onward.start()

    @pl.when(me > 0)
    def send_head():
        back.start()

    top = shift >> LANE_BITS
    lanes = shift & (LANES - 1)

    def own(a, b):
        there = b * BLOCK + PAD + top
        return moved(state[a, pl.ds(there, BLOCK), :], state[a, pl.ds(there + 1, BLOCK), :], lanes)

    def inner(b, carry):
        here = pl.multiple_of(b * BLOCK, BLOCK)
        for a in range(4):
            placed[a, pl.ds(here, BLOCK), :] = own(a, b)
        return carry

    lax.fori_loop(1, blocks - 3, inner, 0, unroll=3)
    for a in range(4):
        before[a, BLOCK:EDGE, :] = state[a, PAD : PAD + EDGE - BLOCK, :]

    new_phase = (-new_low) & (HALF - 1)
    new_base = (new_low + new_phase) >> HALF_BITS
    on_lane = (spot & (segs - 1)) == line
    lows = jnp.sum(jnp.where(on_lane, first - new_base, 0), axis=0, keepdims=True)
    highs = jnp.sum(jnp.where(on_lane, past - new_base, 0), axis=0, keepdims=True)
    block_row = lax.broadcasted_iota(jnp.int32, (BLOCK, LANES), 0)
    lane_group = lane_ids() >> HALF_BITS

    def choose(b, carry):
        here = pl.multiple_of(b * BLOCK, BLOCK)
        for tile in range(2):
            half = 2 * (block_row + b * BLOCK) - 1 + 2 * tile + lane_group
            mask = (half >= lows) & (half < highs)
            chosen[pl.ds(here, BLOCK), tile * LANES : (tile + 1) * LANES] = jnp.where(mask, 1.0, 0.0).astype(
                jnp.bfloat16
            )
        return carry

    lax.fori_loop(0, blocks, choose, 0, unroll=2)
    sums[1:2, :] = jnp.full((1, LANES), new_phase, jnp.int32).astype(jnp.float32)

    @pl.when(me < n - 1)
    def end_right():
        onward.wait_send()
        back.wait_recv()

    @pl.when(me > 0)
    def end_left():
        back.wait_send()
        onward.wait_recv()

    for a in range(4):
        before[a, 0:BLOCK, :] = left_rim[a]
        after[a, PAD : PAD + BLOCK, :] = right_rim[a]
    for a in range(4):
        placed[a, 0:BLOCK, :] = moved(
            before[a, pl.ds(BLOCK + top, BLOCK), :], before[a, pl.ds(BLOCK + top + 1, BLOCK), :], lanes
        )

    for b in range(blocks - 3, blocks):
        offset = b * MARGIN + shift - count
        near = jnp.clip(offset >> LANE_BITS, -PAD, PAD - 7) + PAD
        side = offset & (LANES - 1)
        index = flat + b * MARGIN
        beyond = index + shift >= count
        live = index < new_count
        for a in range(4):
            rim = moved(after[a, pl.ds(near, BLOCK), :], after[a, pl.ds(near + 1, BLOCK), :], side)
            value = jnp.where(beyond, rim, own(a, b))
            placed[a, b * BLOCK : (b + 1) * BLOCK, :] = jnp.where(live, value, 0.0)

    pltpu.make_async_copy(slots, slots, receive).wait()
    sums[0:1, :] = jnp.sum(slots[...], axis=0)
    others = slots.at[pl.ds(0, n - 1)]
    pltpu.make_async_copy(others, others, send).wait()


def apply_kernel(segs, placed, sums, chosen, w_out, m_out, v_out, w_buf, sems):
    m_copy = pltpu.make_async_copy(placed.at[2], m_out, sems.at[0])
    v_copy = pltpu.make_async_copy(placed.at[3], v_out, sems.at[1])
    m_copy.start()
    v_copy.start()
    rows = w_buf.shape[0]
    total = sums[0:1, :]
    phase = sums[1:2, :]
    other = pltpu.roll(total, LANES - segs, 1)
    rate = LEARN * (jnp.sqrt(total) / (jnp.sqrt(other) + EPSILON))
    spot = lane_ids(segs)
    line = lax.broadcasted_iota(jnp.int32, (segs, LANES), 0)
    column = jnp.sum(jnp.where(spot == line, rate, 0.0), axis=1, keepdims=True)
    place = spot.astype(jnp.float32)
    early = place < phase
    late = place >= phase + HALF
    nothing = jnp.zeros((segs, LANES), jnp.float32)
    rates = jnp.concatenate(
        [
            jnp.where(early, column, 0.0),
            jnp.where(early | late, 0.0, column),
            jnp.where(late, column, 0.0),
            nothing,
        ],
        axis=0,
    )
    coarse = rates.astype(jnp.bfloat16)
    fine = (rates - coarse.astype(jnp.float32)).astype(jnp.bfloat16)
    table = jnp.concatenate([coarse, fine], axis=1)
    step = 256
    copies = []
    for c, r0 in enumerate(range(0, rows, step)):
        size = min(step, rows - r0)
        product = jnp.dot(chosen[r0 : r0 + size, :], table, preferred_element_type=jnp.float32)
        factor = product[:, :LANES] + product[:, LANES:]
        w_buf[r0 : r0 + size, :] = placed[0, r0 : r0 + size, :] - factor * placed[1, r0 : r0 + size, :]
        window = pl.ds(r0, size)
        copy = pltpu.make_async_copy(w_buf.at[window], w_out.at[window], sems.at[2 + c])
        copy.start()
        copies.append(copy)
    for copy in (m_copy, v_copy, *copies):
        copy.wait()


def spec(space):
    return pl.BlockSpec(memory_space=space)


def shards(axis, n, params, first_moment, second_moment, grads, old_bounds, new_bounds, seg_start):
    cap = params.shape[0]
    rows = cap // LANES
    f32 = jnp.float32
    flat = [x.reshape(rows, LANES) for x in (params, first_moment, second_moment, grads)]
    segs = seg_start.shape[0]
    tables = (old_bounds, new_bounds, seg_start.reshape(1, segs))
    old_bounds, new_bounds, starts_row, *flat = (
        pltpu.with_memory_space_constraint(x, pltpu.HBM) for x in (*tables, *flat)
    )
    padded = -(-rows // LANES) * LANES
    vmem, hbm = spec(pltpu.VMEM), spec(pltpu.HBM)
    bounds = pltpu.SMEM(old_bounds.shape, jnp.int32)
    starts = pltpu.VMEM((1, segs), jnp.int32)
    rim = pltpu.VMEM((4, BLOCK, LANES), f32)
    dma = pltpu.SemaphoreType.DMA
    placed, sums, chosen = pl.pallas_call(
        functools.partial(step_kernel, axis, n),
        name="step",
        out_shape=(
            jax.ShapeDtypeStruct((4, rows, LANES), f32),
            jax.ShapeDtypeStruct((2, LANES), f32),
            jax.ShapeDtypeStruct((rows, 2 * LANES), jnp.bfloat16),
        ),
        in_specs=[hbm] * 7,
        out_specs=(vmem,) * 3,
        scratch_shapes=[
            pltpu.VMEM((4, rows + 2 * PAD, LANES), f32),
            pltpu.VMEM((rows, LANES), f32),
            pltpu.VMEM((rows, LANES), f32),
            pltpu.VMEM((rows, LANES), grads.dtype),
            pltpu.VMEM((3 * segs, padded), jnp.bfloat16),
            pltpu.VMEM((1, LANES), f32),
            rim,
            rim,
            rim,
            rim,
            pltpu.VMEM((4, EDGE, LANES), f32),
            pltpu.VMEM((4, EDGE, LANES), f32),
            pltpu.VMEM((n, 1, LANES), f32),
            bounds,
            bounds,
            starts,
            dma((4, 2)),
            dma((3,)),
            dma,
            dma,
            dma((2,)),
            dma((2,)),
        ],
        compiler_params=pltpu.CompilerParams(
            collective_id=0, has_side_effects=True, vmem_limit_bytes=VMEM_LIMIT
        ),
    )(old_bounds, new_bounds, starts_row, *flat)
    whole = jax.ShapeDtypeStruct((rows, LANES), f32)
    outs = pl.pallas_call(
        functools.partial(apply_kernel, segs),
        name="apply",
        out_shape=(whole,) * 3,
        in_specs=[vmem] * 3,
        out_specs=(hbm,) * 3,
        scratch_shapes=[pltpu.VMEM((rows, LANES), f32), dma((2 + -(-rows // 256),))],
        compiler_params=pltpu.CompilerParams(vmem_limit_bytes=VMEM_LIMIT),
    )(placed, sums, chosen)
    return tuple(x.reshape(cap) for x in outs)


def solution(mesh):
    (axis,) = mesh.axis_names
    n = mesh.shape[axis]
    placed = (P(axis), P(axis), P(axis), P(axis), P(), P(), P())
    return jax.shard_map(
        functools.partial(shards, axis, n),
        mesh=mesh,
        in_specs=placed,
        out_specs=(P(axis), P(axis), P(axis)),
        check_vma=False,
    )
```

```python
import functools

import jax
import jax.numpy as jnp
from jax import lax
from jax.experimental import pallas as pl
from jax.experimental.pallas import tpu as pltpu
from jax.sharding import PartitionSpec as P

MARGIN = 4096
LANES = 128
BLOCK = MARGIN // LANES
HALF = 64
HALF_BITS = 6
LANE_BITS = 7
PAD = BLOCK + 8
EDGE = 2 * PAD + BLOCK
TILE = 256
REACH = 4


BETA_ONE = 0.9
BETA_TWO = 0.999
CORR_ONE = 1.0 - 0.9**10
CORR_TWO = 1.0 - 0.999**10
DECAY = 0.01
LEARN = 0.1
EPSILON = 1e-06

MESH = pl.DeviceIdType.MESH
VMEM_LIMIT = 16 * 1024 * 1024


def lane_ids(rows=BLOCK):
    return lax.broadcasted_iota(jnp.int32, (rows, LANES), 1)


def flat_ids():
    return lax.broadcasted_iota(jnp.int32, (BLOCK, LANES), 0) * LANES + lane_ids()


def moved(first, second, lanes):
    picked = jnp.where(lane_ids() >= lanes, first, second)
    return pltpu.roll(picked, (LANES - lanes) & (LANES - 1), 1)


def fetched(tables, refs, sems):
    copies = [pltpu.make_async_copy(t, r, sems.at[i]) for i, (t, r) in enumerate(zip(tables, refs))]
    for copy in copies:
        copy.start()
    return copies


def step_kernel(
    axis, n, old_hbm, new_hbm, seg_hbm, w_hbm, m_hbm, v_hbm, g_hbm, placed, sums, chosen, wide,
    state, m_buf, v_buf, g_buf, member, part, tail, head, left_rim, right_rim,
    before, after, slots, old_ref, new_ref, seg_ref, seg_list, sems, table_sems, send, receive, rim_send, rim_receive,
):
    rows = m_buf.shape[0]
    blocks = rows // BLOCK
    segs = seg_ref.shape[1]
    me = lax.axis_index(axis)
    right = lax.rem(me + 1, n)
    left = lax.rem(me + n - 1, n)
    tables = fetched((old_hbm, new_hbm, seg_hbm, seg_hbm), (old_ref, new_ref, seg_ref, seg_list), table_sems)
    weights = state.at[0, pl.ds(PAD, rows)]
    loads = fetched((g_hbm, m_hbm, v_hbm, w_hbm), (g_buf, m_buf, v_buf, weights), sems)
    barrier = pltpu.get_barrier_semaphore()
    near = [k for k in range(-REACH, REACH + 1) if k and abs(k) < n]

    def inside(k):
        return (me + k >= 0) & (me + k < n)

    for k in near:

        @pl.when(inside(k))
        def greet(k=k):
            pl.semaphore_signal(barrier, inc=1, device_id=(me + k,), device_id_type=MESH)

    for copy in tables:
        copy.wait()
    low = old_ref[me]
    count = old_ref[me + 1] - low
    new_low = new_ref[me]
    new_count = new_ref[me + 1] - new_low
    shift = new_low - low
    phase = (-low) & (HALF - 1)
    spot = lane_ids(segs)
    line = lax.broadcasted_iota(jnp.int32, (segs, LANES), 0)
    square_line = lax.broadcasted_iota(jnp.int32, (segs, segs), 0)
    square_spot = lax.broadcasted_iota(jnp.int32, (segs, segs), 1)
    starts = (seg_ref[...] >> HALF_BITS).astype(jnp.float32)
    first = jnp.sum(jnp.where(square_spot == square_line, starts, 0.0), axis=1, keepdims=True)
    past = jnp.sum(jnp.where(square_spot == square_line + 1, starts, 0.0), axis=1, keepdims=True)
    past = jnp.where(square_line[:, :1] == segs - 1, 4.0 * n * rows, past)
    first = jnp.broadcast_to(first.astype(jnp.int32), (segs, LANES))
    past = jnp.broadcast_to(past.astype(jnp.int32), (segs, LANES))
    base = (low + phase) >> HALF_BITS
    first_half = first - base
    past_half = past - base
    padded = member.shape[1]
    for group in range(3):
        for tile in range(padded // LANES):
            half = 2 * (spot + tile * LANES) - 1 + group
            mask = (half >= first_half) & (half < past_half)
            member[group * segs : (group + 1) * segs, tile * LANES : (tile + 1) * LANES] = jnp.where(
                mask, 1.0, 0.0
            ).astype(jnp.bfloat16)

    flat = flat_ids()

    for copy in loads[:3]:
        copy.wait()
    for r0 in range(0, rows, BLOCK):
        here = slice(r0, r0 + BLOCK)
        there = slice(r0 + PAD, r0 + PAD + BLOCK)
        gradient = g_buf[here, :].astype(jnp.float32)
        moment = BETA_ONE * m_buf[here, :] + (1.0 - BETA_ONE) * gradient
        second = BETA_TWO * v_buf[here, :] + ((1.0 - BETA_TWO) * gradient) * gradient
        spread = second * (CORR_ONE * CORR_ONE / CORR_TWO)
        state[1, there, :] = moment / (spread * lax.rsqrt(spread) + CORR_ONE * EPSILON)
        state[2, there, :] = moment
        state[3, there, :] = second
    loads[3].wait()
    product = None
    for t0 in range(0, rows, TILE):
        t1 = min(t0 + TILE, rows)
        pieces = [[], [], [], []]
        for r0 in range(t0, t1, BLOCK):
            there = slice(r0 + PAD, r0 + PAD + BLOCK)
            weight = state[0, there, :]
            update = state[1, there, :] + DECAY * weight
            state[1, there, :] = update
            for i, value in enumerate((weight, update)):
                square = value * value
                if r0 + 2 * BLOCK >= rows:
                    square = jnp.where(flat + r0 * LANES < count, square, 0.0)
                coarse = square.astype(jnp.bfloat16)
                pieces[i].append(coarse)
                pieces[i + 2].append((square - coarse.astype(jnp.float32)).astype(jnp.bfloat16))
        squares = jnp.concatenate([jnp.concatenate(p, axis=0) for p in pieces], axis=1)
        partial = jnp.dot(member[:, t0:t1], squares, preferred_element_type=jnp.float32)
        product = partial if product is None else product + partial
    product = product[:, : 2 * LANES] + product[:, 2 * LANES :]
    on_lane = (spot & (segs - 1)) == line
    for i in range(2):
        columns = slice(i * LANES, (i + 1) * LANES)
        mixed = jnp.where(
            spot < phase,
            product[0:segs, columns],
            jnp.where(
                spot < phase + HALF, product[segs : 2 * segs, columns], product[2 * segs : 3 * segs, columns]
            ),
        )
        column = jnp.sum(mixed, axis=1, keepdims=True)
        part[i : i + 1, :] = jnp.sum(jnp.where(on_lane, column, 0.0), axis=0, keepdims=True)
    pl.semaphore_wait(barrier, jnp.minimum(me, REACH) + jnp.minimum(n - 1 - me, REACH))

    def tell(k):
        return pltpu.make_async_remote_copy(
            src_ref=part,
            dst_ref=slots.at[k + REACH],
            send_sem=send.at[k + REACH],
            recv_sem=receive.at[k + REACH],
            device_id=(me + k,),
            device_id_type=MESH,
        )

    onward = pltpu.make_async_remote_copy(
        src_ref=tail,
        dst_ref=left_rim,
        send_sem=rim_send.at[0],
        recv_sem=rim_receive.at[0],
        device_id=(right,),
        device_id_type=MESH,
    )
    back = pltpu.make_async_remote_copy(
        src_ref=head,
        dst_ref=right_rim,
        send_sem=rim_send.at[1],
        recv_sem=rim_receive.at[1],
        device_id=(left,),
        device_id_type=MESH,
    )

    for k in near:

        @pl.when(inside(k))
        def send_sums(k=k):
            tell(k).start()

    sums[3:5, :] = part[...]

    start = count - MARGIN
    start_row = start >> LANE_BITS
    start_lane = start & (LANES - 1)
    for a in range(4):
        head[a] = state[a, PAD : PAD + BLOCK, :]
        tail[a] = moved(
            state[a, pl.ds(PAD + start_row, BLOCK), :],
            state[a, pl.ds(PAD + start_row + 1, BLOCK), :],
            start_lane,
        )

    @pl.when(me < n - 1)
    def send_tail():
        onward.start()

    @pl.when(me > 0)
    def send_head():
        back.start()

    top = shift >> LANE_BITS
    lanes = shift & (LANES - 1)

    def own(a, b):
        there = b * BLOCK + PAD + top
        return moved(state[a, pl.ds(there, BLOCK), :], state[a, pl.ds(there + 1, BLOCK), :], lanes)

    def inner(b, carry):
        here = pl.multiple_of(b * BLOCK, BLOCK)
        for a in range(4):
            placed[a, pl.ds(here, BLOCK), :] = own(a, b)
        return carry

    lax.fori_loop(1, blocks - 3, inner, 0, unroll=3)
    for a in range(4):
        before[a, BLOCK:EDGE, :] = state[a, PAD : PAD + EDGE - BLOCK, :]

    new_phase = (-new_low) & (HALF - 1)
    new_base = (new_low + new_phase) >> HALF_BITS
    lows = jnp.sum(jnp.where(on_lane, first - new_base, 0), axis=0, keepdims=True)
    highs = jnp.sum(jnp.where(on_lane, past - new_base, 0), axis=0, keepdims=True)
    block_row = lax.broadcasted_iota(jnp.int32, (BLOCK, LANES), 0)
    lane_group = lane_ids() >> HALF_BITS

    def choose(b, carry):
        here = pl.multiple_of(b * BLOCK, BLOCK)
        for tile in range(2):
            half = 2 * (block_row + b * BLOCK) - 1 + 2 * tile + lane_group
            mask = (half >= lows) & (half < highs)
            chosen[pl.ds(here, BLOCK), tile * LANES : (tile + 1) * LANES] = jnp.where(mask, 1.0, 0.0).astype(
                jnp.bfloat16
            )
        return carry

    lax.fori_loop(0, blocks, choose, 0, unroll=2)
    sums[2:3, :] = jnp.full((1, LANES), new_phase, jnp.int32).astype(jnp.float32)

    def longest(s, most):
        return jnp.maximum(most, seg_list[0, s + 1] - seg_list[0, s])

    most = lax.fori_loop(0, segs - 1, longest, old_ref[n] - seg_list[0, segs - 1], unroll=9)
    wide[0] = jnp.where(most > REACH * (rows * LANES - 2 * MARGIN) - MARGIN, 1, 0)

    @pl.when(me < n - 1)
    def end_right():
        onward.wait_send()
        back.wait_recv()

    @pl.when(me > 0)
    def end_left():
        back.wait_send()
        onward.wait_recv()

    for a in range(4):
        before[a, 0:BLOCK, :] = left_rim[a]
        after[a, PAD : PAD + BLOCK, :] = right_rim[a]
    for a in range(4):
        placed[a, 0:BLOCK, :] = moved(
            before[a, pl.ds(BLOCK + top, BLOCK), :], before[a, pl.ds(BLOCK + top + 1, BLOCK), :], lanes
        )

    for b in range(blocks - 3, blocks):
        offset = b * MARGIN + shift - count
        edge = jnp.clip(offset >> LANE_BITS, -PAD, PAD - 7) + PAD
        side = offset & (LANES - 1)
        index = flat + b * MARGIN
        beyond = index + shift >= count
        live = index < new_count
        for a in range(4):
            rim = moved(after[a, pl.ds(edge, BLOCK), :], after[a, pl.ds(edge + 1, BLOCK), :], side)
            value = jnp.where(beyond, rim, own(a, b))
            placed[a, b * BLOCK : (b + 1) * BLOCK, :] = jnp.where(live, value, 0.0)

    total = part[...]
    for k in near:

        @pl.when(inside(-k))
        def get_sums(k=k):
            tell(k).wait_recv()

        total = total + jnp.where(inside(-k), slots[k + REACH], 0.0)
    sums[0:2, :] = total
    for k in near:

        @pl.when(inside(k))
        def end_sums(k=k):
            tell(k).wait_send()


def everyone_kernel(axis, n, near_sums, sums, part, slots, send, receive):
    me = lax.axis_index(axis)
    barrier = pltpu.get_barrier_semaphore()

    def greet(k, carry):
        pl.semaphore_signal(barrier, inc=1, device_id=(lax.rem(me + k, n),), device_id_type=MESH)
        return carry

    lax.fori_loop(1, n, greet, 0)
    part[...] = near_sums[3:5, :]
    sums[2:5, :] = near_sums[2:5, :]
    pl.semaphore_wait(barrier, n - 1)

    def tell(k, carry):
        pltpu.make_async_remote_copy(
            src_ref=part,
            dst_ref=slots.at[me],
            send_sem=send,
            recv_sem=receive,
            device_id=(lax.rem(me + k, n),),
            device_id_type=MESH,
        ).start()
        return carry

    lax.fori_loop(1, n, tell, 0)
    pltpu.make_async_copy(part, slots.at[me], receive).start()
    pltpu.make_async_copy(slots, slots, receive).wait()
    sums[0:2, :] = jnp.sum(slots[...], axis=0)
    others = slots.at[pl.ds(0, n - 1)]
    pltpu.make_async_copy(others, others, send).wait()


def apply_kernel(segs, placed, sums, chosen, w_out, m_out, v_out, w_buf, sems):
    m_copy = pltpu.make_async_copy(placed.at[2], m_out, sems.at[0])
    v_copy = pltpu.make_async_copy(placed.at[3], v_out, sems.at[1])
    m_copy.start()
    v_copy.start()
    rows = w_buf.shape[0]
    total = sums[0:1, :]
    other = sums[1:2, :]
    phase = sums[2:3, :]
    rate = LEARN * (jnp.sqrt(total) / (jnp.sqrt(other) + EPSILON))
    place = lax.broadcasted_iota(jnp.int32, (LANES, LANES), 0).astype(jnp.float32)
    lower = lane_ids(LANES) < segs
    early = place < phase
    late = place >= phase + HALF
    rates = jnp.concatenate(
        [
            jnp.where((lower & early) | ~(lower | early | late), rate, 0.0),
            jnp.where(lower & late, rate, 0.0),
        ],
        axis=1,
    )
    coarse = rates.astype(jnp.bfloat16)
    fine = (rates - coarse.astype(jnp.float32)).astype(jnp.bfloat16)
    table = jnp.concatenate([coarse, fine], axis=0)
    step = 256
    copies = []
    for c, r0 in enumerate(range(0, rows, step)):
        size = min(step, rows - r0)
        product = lax.dot_general(
            chosen[r0 : r0 + size, :], table, (((1,), (1,)), ((), ())), preferred_element_type=jnp.float32
        )
        factor = product[:, :LANES] + product[:, LANES:]
        w_buf[r0 : r0 + size, :] = placed[0, r0 : r0 + size, :] - factor * placed[1, r0 : r0 + size, :]
        window = pl.ds(r0, size)
        copy = pltpu.make_async_copy(w_buf.at[window], w_out.at[window], sems.at[2 + c])
        copy.start()
        copies.append(copy)
    for copy in (m_copy, v_copy, *copies):
        copy.wait()


def spec(space):
    return pl.BlockSpec(memory_space=space)


def shards(axis, n, params, first_moment, second_moment, grads, old_bounds, new_bounds, seg_start):
    cap = params.shape[0]
    rows = cap // LANES
    f32 = jnp.float32
    flat = [x.reshape(rows, LANES) for x in (params, first_moment, second_moment, grads)]
    segs = seg_start.shape[0]
    tables = (old_bounds, new_bounds, seg_start.reshape(1, segs))
    old_bounds, new_bounds, starts_row, *flat = (
        pltpu.with_memory_space_constraint(x, pltpu.HBM) for x in (*tables, *flat)
    )
    padded = -(-rows // LANES) * LANES
    vmem, hbm = spec(pltpu.VMEM), spec(pltpu.HBM)
    bounds = pltpu.SMEM(old_bounds.shape, jnp.int32)
    starts = pltpu.VMEM((1, segs), jnp.int32)
    rim = pltpu.VMEM((4, BLOCK, LANES), f32)
    dma = pltpu.SemaphoreType.DMA
    placed, sums, chosen, wide = pl.pallas_call(
        functools.partial(step_kernel, axis, n),
        name="step",
        out_shape=(
            jax.ShapeDtypeStruct((4, rows, LANES), f32),
            jax.ShapeDtypeStruct((5, LANES), f32),
            jax.ShapeDtypeStruct((rows, 2 * LANES), jnp.bfloat16),
            jax.ShapeDtypeStruct((1,), jnp.int32),
        ),
        in_specs=[hbm] * 7,
        out_specs=(vmem, vmem, vmem, spec(pltpu.SMEM)),
        scratch_shapes=[
            pltpu.VMEM((4, rows + 2 * PAD, LANES), f32),
            pltpu.VMEM((rows, LANES), f32),
            pltpu.VMEM((rows, LANES), f32),
            pltpu.VMEM((rows, LANES), grads.dtype),
            pltpu.VMEM((3 * segs, padded), jnp.bfloat16),
            pltpu.VMEM((2, LANES), f32),
            rim,
            rim,
            rim,
            rim,
            pltpu.VMEM((4, EDGE, LANES), f32),
            pltpu.VMEM((4, EDGE, LANES), f32),
            pltpu.VMEM((2 * REACH + 1, 2, LANES), f32),
            bounds,
            bounds,
            starts,
            pltpu.SMEM((1, segs), jnp.int32),
            dma((4,)),
            dma((4,)),
            dma((2 * REACH + 1,)),
            dma((2 * REACH + 1,)),
            dma((2,)),
            dma((2,)),
        ],
        compiler_params=pltpu.CompilerParams(
            collective_id=0, has_side_effects=True, vmem_limit_bytes=VMEM_LIMIT
        ),
    )(old_bounds, new_bounds, starts_row, *flat)
    whole = jax.ShapeDtypeStruct((rows, LANES), f32)
    def finish(placed, sums, chosen):
        return pl.pallas_call(
            functools.partial(apply_kernel, segs),
            name="apply",
            out_shape=(whole,) * 3,
            in_specs=[vmem] * 3,
            out_specs=(hbm,) * 3,
            scratch_shapes=[pltpu.VMEM((rows, LANES), f32), dma((2 + -(-rows // 256),))],
            compiler_params=pltpu.CompilerParams(vmem_limit_bytes=VMEM_LIMIT),
        )(placed, sums, chosen)

    def gather(placed, sums, chosen):
        sums = pl.pallas_call(
            functools.partial(everyone_kernel, axis, n),
            name="everyone",
            out_shape=jax.ShapeDtypeStruct((5, LANES), f32),
            in_specs=[vmem],
            out_specs=vmem,
            scratch_shapes=[pltpu.VMEM((2, LANES), f32), pltpu.VMEM((n, 2, LANES), f32), dma, dma],
            compiler_params=pltpu.CompilerParams(
                collective_id=1, has_side_effects=True, vmem_limit_bytes=VMEM_LIMIT
            ),
        )(sums)
        return finish(placed, sums, chosen)

    outs = lax.switch(wide.reshape(()), (finish, gather), placed, sums, chosen)
    return tuple(x.reshape(cap) for x in outs)


def solution(mesh):
    (axis,) = mesh.axis_names
    n = mesh.shape[axis]
    placed = (P(axis), P(axis), P(axis), P(axis), P(), P(), P())
    return jax.shard_map(
        functools.partial(shards, axis, n),
        mesh=mesh,
        in_specs=placed,
        out_specs=(P(axis), P(axis), P(axis)),
        check_vma=False,
    )
```

```python
import functools

import jax
import jax.numpy as jnp
from jax import lax
from jax.experimental import pallas as pl
from jax.experimental.pallas import tpu as pltpu
from jax.sharding import PartitionSpec as P

MARGIN = 4096
LANES = 128
BLOCK = MARGIN // LANES
HALF = 64
HALF_BITS = 6
LANE_BITS = 7
PAD = BLOCK + 8
EDGE = 2 * PAD + BLOCK
TILE = 256
REACH = 4
UPDATE, WEIGHT, MOMENT, SECOND = range(4)


BETA_ONE = 0.9
BETA_TWO = 0.999
CORR_ONE = 1.0 - 0.9**10
CORR_TWO = 1.0 - 0.999**10
DECAY = 0.01
LEARN = 0.1
EPSILON = 1e-06

MESH = pl.DeviceIdType.MESH
VMEM_LIMIT = 16 * 1024 * 1024


def lane_ids(rows=BLOCK):
    return lax.broadcasted_iota(jnp.int32, (rows, LANES), 1)


def flat_ids():
    return lax.broadcasted_iota(jnp.int32, (BLOCK, LANES), 0) * LANES + lane_ids()


def moved(first, second, lanes):
    picked = jnp.where(lane_ids() >= lanes, first, second)
    return pltpu.roll(picked, (LANES - lanes) & (LANES - 1), 1)


def adaptive(moment, second):
    spread = second * (CORR_ONE * CORR_ONE / CORR_TWO)
    return moment / (spread * lax.rsqrt(spread) + CORR_ONE * EPSILON)


def fetched(tables, refs, sems):
    copies = [pltpu.make_async_copy(t, r, sems.at[i]) for i, (t, r) in enumerate(zip(tables, refs))]
    for copy in copies:
        copy.start()
    return copies


def step_kernel(
    axis, n, old_hbm, new_hbm, seg_hbm, w_hbm, m_hbm, v_hbm, g_hbm, placed, sums, chosen, wide,
    state, m_buf, v_buf, g_buf, member, part, tail, left_rim, right_rim,
    before, after, slots, old_ref, new_ref, seg_ref, seg_list, sems, table_sems, send, receive, rim_send, rim_receive,
):
    rows = m_buf.shape[0]
    blocks = rows // BLOCK
    segs = seg_ref.shape[1]
    me = lax.axis_index(axis)
    right = lax.rem(me + 1, n)
    left = lax.rem(me + n - 1, n)
    tables = fetched((old_hbm, new_hbm, seg_hbm, seg_hbm), (old_ref, new_ref, seg_ref, seg_list), table_sems)
    weights = state.at[WEIGHT, pl.ds(PAD, rows)]
    loads = fetched((g_hbm, m_hbm, v_hbm, w_hbm), (g_buf, m_buf, v_buf, weights), sems)
    barrier = pltpu.get_barrier_semaphore()
    near = [k for k in range(-REACH, REACH + 1) if k and abs(k) < n]

    def inside(k):
        return (me + k >= 0) & (me + k < n)

    for k in near:

        @pl.when(inside(k))
        def greet(k=k):
            pl.semaphore_signal(barrier, inc=1, device_id=(me + k,), device_id_type=MESH)

    for copy in tables:
        copy.wait()
    low = old_ref[me]
    count = old_ref[me + 1] - low
    new_low = new_ref[me]
    new_count = new_ref[me + 1] - new_low
    shift = new_low - low
    phase = (-low) & (HALF - 1)
    spot = lane_ids(segs)
    line = lax.broadcasted_iota(jnp.int32, (segs, LANES), 0)
    square_line = lax.broadcasted_iota(jnp.int32, (segs, segs), 0)
    square_spot = lax.broadcasted_iota(jnp.int32, (segs, segs), 1)
    starts = (seg_ref[...] >> HALF_BITS).astype(jnp.float32)
    first = jnp.sum(jnp.where(square_spot == square_line, starts, 0.0), axis=1, keepdims=True)
    past = jnp.sum(jnp.where(square_spot == square_line + 1, starts, 0.0), axis=1, keepdims=True)
    past = jnp.where(square_line[:, :1] == segs - 1, 4.0 * n * rows, past)
    first = jnp.broadcast_to(first.astype(jnp.int32), (segs, LANES))
    past = jnp.broadcast_to(past.astype(jnp.int32), (segs, LANES))
    base = (low + phase) >> HALF_BITS
    first_half = first - base
    past_half = past - base
    padded = member.shape[1]
    for group in range(3):
        for tile in range(padded // LANES):
            half = 2 * (spot + tile * LANES) - 1 + group
            mask = (half >= first_half) & (half < past_half)
            member[group * segs : (group + 1) * segs, tile * LANES : (tile + 1) * LANES] = jnp.where(
                mask, 1.0, 0.0
            ).astype(jnp.bfloat16)

    flat = flat_ids()

    for copy in loads[:3]:
        copy.wait()
    for r0 in range(0, rows, BLOCK):
        here = slice(r0, r0 + BLOCK)
        there = slice(r0 + PAD, r0 + PAD + BLOCK)
        gradient = g_buf[here, :].astype(jnp.float32)
        moment = BETA_ONE * m_buf[here, :] + (1.0 - BETA_ONE) * gradient
        second = BETA_TWO * v_buf[here, :] + ((1.0 - BETA_TWO) * gradient) * gradient
        state[UPDATE, there, :] = adaptive(moment, second)
        state[MOMENT, there, :] = moment
        state[SECOND, there, :] = second
    loads[3].wait()
    pl.semaphore_wait(barrier, jnp.minimum(me, REACH) + jnp.minimum(n - 1 - me, REACH))
    start = count - MARGIN
    start_row = start >> LANE_BITS
    start_lane = start & (LANES - 1)
    for a in range(3):
        tail[a] = moved(
            state[a + 1, pl.ds(PAD + start_row, BLOCK), :],
            state[a + 1, pl.ds(PAD + start_row + 1, BLOCK), :],
            start_lane,
        )
    onward = pltpu.make_async_remote_copy(
        src_ref=tail,
        dst_ref=left_rim,
        send_sem=rim_send.at[0],
        recv_sem=rim_receive.at[0],
        device_id=(right,),
        device_id_type=MESH,
    )
    back = pltpu.make_async_remote_copy(
        src_ref=state.at[pl.ds(1, 3), pl.ds(PAD, BLOCK)],
        dst_ref=right_rim,
        send_sem=rim_send.at[1],
        recv_sem=rim_receive.at[1],
        device_id=(left,),
        device_id_type=MESH,
    )

    @pl.when(me < n - 1)
    def send_tail():
        onward.start()

    @pl.when(me > 0)
    def send_head():
        back.start()

    product = None
    for t0 in range(0, rows, TILE):
        t1 = min(t0 + TILE, rows)
        pieces = [[], [], [], []]
        for r0 in range(t0, t1, BLOCK):
            there = slice(r0 + PAD, r0 + PAD + BLOCK)
            weight = state[WEIGHT, there, :]
            update = state[UPDATE, there, :] + DECAY * weight
            state[UPDATE, there, :] = update
            for i, value in enumerate((weight, update)):
                square = value * value
                if r0 + 2 * BLOCK >= rows:
                    square = jnp.where(flat + r0 * LANES < count, square, 0.0)
                coarse = square.astype(jnp.bfloat16)
                pieces[i].append(coarse)
                pieces[i + 2].append((square - coarse.astype(jnp.float32)).astype(jnp.bfloat16))
        squares = jnp.concatenate([jnp.concatenate(p, axis=0) for p in pieces], axis=1)
        partial = jnp.dot(member[:, t0:t1], squares, preferred_element_type=jnp.float32)
        product = partial if product is None else product + partial
    product = product[:, : 2 * LANES] + product[:, 2 * LANES :]
    on_lane = (spot & (segs - 1)) == line
    for i in range(2):
        columns = slice(i * LANES, (i + 1) * LANES)
        mixed = jnp.where(
            spot < phase,
            product[0:segs, columns],
            jnp.where(
                spot < phase + HALF, product[segs : 2 * segs, columns], product[2 * segs : 3 * segs, columns]
            ),
        )
        column = jnp.sum(mixed, axis=1, keepdims=True)
        part[i : i + 1, :] = jnp.sum(jnp.where(on_lane, column, 0.0), axis=0, keepdims=True)

    def tell(k):
        return pltpu.make_async_remote_copy(
            src_ref=part,
            dst_ref=slots.at[k + REACH],
            send_sem=send.at[k + REACH],
            recv_sem=receive.at[k + REACH],
            device_id=(me + k,),
            device_id_type=MESH,
        )

    for k in near:

        @pl.when(inside(k))
        def send_sums(k=k):
            tell(k).start()

    sums[3:5, :] = part[...]

    top = shift >> LANE_BITS
    lanes = shift & (LANES - 1)

    def own(a, b):
        there = b * BLOCK + PAD + top
        return moved(state[a, pl.ds(there, BLOCK), :], state[a, pl.ds(there + 1, BLOCK), :], lanes)

    def inner(b, carry):
        here = pl.multiple_of(b * BLOCK, BLOCK)
        for a in range(4):
            placed[a, pl.ds(here, BLOCK), :] = own(a, b)
        return carry

    lax.fori_loop(1, blocks - 3, inner, 0, unroll=3)
    for a in range(4):
        before[a, BLOCK:EDGE, :] = state[a, PAD : PAD + EDGE - BLOCK, :]
    for b in range(blocks - 3, blocks):
        live = flat + b * MARGIN < new_count
        for a in range(4):
            placed[a, b * BLOCK : (b + 1) * BLOCK, :] = jnp.where(live, own(a, b), 0.0)

    new_phase = (-new_low) & (HALF - 1)
    new_base = (new_low + new_phase) >> HALF_BITS
    lows = jnp.sum(jnp.where(on_lane, first - new_base, 0), axis=0, keepdims=True)
    highs = jnp.sum(jnp.where(on_lane, past - new_base, 0), axis=0, keepdims=True)
    block_row = lax.broadcasted_iota(jnp.int32, (BLOCK, LANES), 0)
    lane_group = lane_ids() >> HALF_BITS

    def choose(b, carry):
        here = pl.multiple_of(b * BLOCK, BLOCK)
        for tile in range(2):
            half = 2 * (block_row + b * BLOCK) - 1 + 2 * tile + lane_group
            mask = (half >= lows) & (half < highs)
            chosen[pl.ds(here, BLOCK), tile * LANES : (tile + 1) * LANES] = jnp.where(mask, 1.0, 0.0).astype(
                jnp.bfloat16
            )
        return carry

    lax.fori_loop(0, blocks, choose, 0, unroll=2)
    sums[2:3, :] = jnp.full((1, LANES), new_phase, jnp.int32).astype(jnp.float32)

    def longest(s, most):
        return jnp.maximum(most, seg_list[0, s + 1] - seg_list[0, s])

    most = lax.fori_loop(0, segs - 1, longest, old_ref[n] - seg_list[0, segs - 1], unroll=9)
    wide[...] = jnp.full((1, LANES), jnp.where(most > REACH * (rows * LANES - 2 * MARGIN) - MARGIN, 1, 0), jnp.int32)

    @pl.when(me < n - 1)
    def end_right():
        onward.wait_send()
        back.wait_recv()

    @pl.when(me > 0)
    def end_left():
        back.wait_send()
        onward.wait_recv()

    for ref, there, rim in ((before, slice(0, BLOCK), left_rim), (after, slice(PAD, PAD + BLOCK), right_rim)):
        for a in range(3):
            ref[a + 1, there, :] = rim[a]
        ref[UPDATE, there, :] = adaptive(rim[1], rim[2]) + DECAY * rim[0]
    for a in range(4):
        placed[a, 0:BLOCK, :] = moved(
            before[a, pl.ds(BLOCK + top, BLOCK), :], before[a, pl.ds(BLOCK + top + 1, BLOCK), :], lanes
        )

    for b in range(blocks - 3, blocks):
        offset = b * MARGIN + shift - count
        edge = jnp.clip(offset >> LANE_BITS, -PAD, PAD - 7) + PAD
        side = offset & (LANES - 1)
        index = flat + b * MARGIN
        beyond = (index + shift >= count) & (index < new_count)
        here = slice(b * BLOCK, (b + 1) * BLOCK)
        for a in range(4):
            rim = moved(after[a, pl.ds(edge, BLOCK), :], after[a, pl.ds(edge + 1, BLOCK), :], side)
            placed[a, here, :] = jnp.where(beyond, rim, placed[a, here, :])

    total = part[...]
    for k in near:

        @pl.when(inside(-k))
        def get_sums(k=k):
            tell(k).wait_recv()

        total = total + jnp.where(inside(-k), slots[k + REACH], 0.0)
    sums[0:2, :] = total
    for k in near:

        @pl.when(inside(k))
        def end_sums(k=k):
            tell(k).wait_send()


def everyone_kernel(axis, n, near_sums, sums, part, slots, send, receive):
    me = lax.axis_index(axis)
    barrier = pltpu.get_barrier_semaphore()

    def greet(k, carry):
        pl.semaphore_signal(barrier, inc=1, device_id=(lax.rem(me + k, n),), device_id_type=MESH)
        return carry

    lax.fori_loop(1, n, greet, 0)
    part[...] = near_sums[3:5, :]
    sums[2:5, :] = near_sums[2:5, :]
    pl.semaphore_wait(barrier, n - 1)

    def tell(k, carry):
        pltpu.make_async_remote_copy(
            src_ref=part,
            dst_ref=slots.at[me],
            send_sem=send,
            recv_sem=receive,
            device_id=(lax.rem(me + k, n),),
            device_id_type=MESH,
        ).start()
        return carry

    lax.fori_loop(1, n, tell, 0)
    pltpu.make_async_copy(part, slots.at[me], receive).start()
    pltpu.make_async_copy(slots, slots, receive).wait()
    sums[0:2, :] = jnp.sum(slots[...], axis=0)
    others = slots.at[pl.ds(0, n - 1)]
    pltpu.make_async_copy(others, others, send).wait()


def apply_kernel(segs, placed, sums, chosen, w_out, m_out, v_out, w_buf, sems):
    m_copy = pltpu.make_async_copy(placed.at[MOMENT], m_out, sems.at[0])
    v_copy = pltpu.make_async_copy(placed.at[SECOND], v_out, sems.at[1])
    m_copy.start()
    v_copy.start()
    rows = w_buf.shape[0]
    total = sums[0:1, :]
    other = sums[1:2, :]
    phase = sums[2:3, :]
    rate = LEARN * (jnp.sqrt(total) / (jnp.sqrt(other) + EPSILON))
    place = lax.broadcasted_iota(jnp.int32, (LANES, LANES), 0).astype(jnp.float32)
    lower = lane_ids(LANES) < segs
    early = place < phase
    late = place >= phase + HALF
    rates = jnp.concatenate(
        [
            jnp.where((lower & early) | ~(lower | early | late), rate, 0.0),
            jnp.where(lower & late, rate, 0.0),
        ],
        axis=1,
    )
    coarse = rates.astype(jnp.bfloat16)
    fine = (rates - coarse.astype(jnp.float32)).astype(jnp.bfloat16)
    table = jnp.concatenate([coarse, fine], axis=0)
    step = 256
    copies = []
    for c, r0 in enumerate(range(0, rows, step)):
        size = min(step, rows - r0)
        product = lax.dot_general(
            chosen[r0 : r0 + size, :], table, (((1,), (1,)), ((), ())), preferred_element_type=jnp.float32
        )
        factor = product[:, :LANES] + product[:, LANES:]
        w_buf[r0 : r0 + size, :] = placed[WEIGHT, r0 : r0 + size, :] - factor * placed[UPDATE, r0 : r0 + size, :]
        window = pl.ds(r0, size)
        copy = pltpu.make_async_copy(w_buf.at[window], w_out.at[window], sems.at[2 + c])
        copy.start()
        copies.append(copy)
    for copy in (m_copy, v_copy, *copies):
        copy.wait()


def spec(space):
    return pl.BlockSpec(memory_space=space)


def shards(axis, n, params, first_moment, second_moment, grads, old_bounds, new_bounds, seg_start):
    cap = params.shape[0]
    rows = cap // LANES
    f32 = jnp.float32
    flat = [x.reshape(rows, LANES) for x in (params, first_moment, second_moment, grads)]
    segs = seg_start.shape[0]
    tables = (old_bounds, new_bounds, seg_start.reshape(1, segs))
    old_bounds, new_bounds, starts_row, *flat = (
        pltpu.with_memory_space_constraint(x, pltpu.HBM) for x in (*tables, *flat)
    )
    padded = -(-rows // LANES) * LANES
    vmem, hbm = spec(pltpu.VMEM), spec(pltpu.HBM)
    bounds = pltpu.SMEM(old_bounds.shape, jnp.int32)
    starts = pltpu.VMEM((1, segs), jnp.int32)
    rim = pltpu.VMEM((3, BLOCK, LANES), f32)
    dma = pltpu.SemaphoreType.DMA
    placed, sums, chosen, wide = pl.pallas_call(
        functools.partial(step_kernel, axis, n),
        name="step",
        out_shape=(
            jax.ShapeDtypeStruct((4, rows, LANES), f32),
            jax.ShapeDtypeStruct((5, LANES), f32),
            jax.ShapeDtypeStruct((rows, 2 * LANES), jnp.bfloat16),
            jax.ShapeDtypeStruct((1, LANES), jnp.int32),
        ),
        in_specs=[hbm] * 7,
        out_specs=(vmem, vmem, vmem, vmem),
        scratch_shapes=[
            pltpu.VMEM((4, rows + 2 * PAD, LANES), f32),
            pltpu.VMEM((rows, LANES), f32),
            pltpu.VMEM((rows, LANES), f32),
            pltpu.VMEM((rows, LANES), grads.dtype),
            pltpu.VMEM((3 * segs, padded), jnp.bfloat16),
            pltpu.VMEM((2, LANES), f32),
            rim,
            rim,
            rim,
            pltpu.VMEM((4, EDGE, LANES), f32),
            pltpu.VMEM((4, EDGE, LANES), f32),
            pltpu.VMEM((2 * REACH + 1, 2, LANES), f32),
            bounds,
            bounds,
            starts,
            pltpu.SMEM((1, segs), jnp.int32),
            dma((4,)),
            dma((4,)),
            dma((2 * REACH + 1,)),
            dma((2 * REACH + 1,)),
            dma((2,)),
            dma((2,)),
        ],
        compiler_params=pltpu.CompilerParams(
            collective_id=0, has_side_effects=True, vmem_limit_bytes=VMEM_LIMIT
        ),
    )(old_bounds, new_bounds, starts_row, *flat)
    whole = jax.ShapeDtypeStruct((rows, LANES), f32)
    def finish(placed, sums, chosen):
        return pl.pallas_call(
            functools.partial(apply_kernel, segs),
            name="apply",
            out_shape=(whole,) * 3,
            in_specs=[vmem] * 3,
            out_specs=(hbm,) * 3,
            scratch_shapes=[pltpu.VMEM((rows, LANES), f32), dma((2 + -(-rows // 256),))],
            compiler_params=pltpu.CompilerParams(vmem_limit_bytes=VMEM_LIMIT),
        )(placed, sums, chosen)

    def gather(placed, sums, chosen):
        sums = pl.pallas_call(
            functools.partial(everyone_kernel, axis, n),
            name="everyone",
            out_shape=jax.ShapeDtypeStruct((5, LANES), f32),
            in_specs=[vmem],
            out_specs=vmem,
            scratch_shapes=[pltpu.VMEM((2, LANES), f32), pltpu.VMEM((n, 2, LANES), f32), dma, dma],
            compiler_params=pltpu.CompilerParams(
                collective_id=1, has_side_effects=True, vmem_limit_bytes=VMEM_LIMIT
            ),
        )(sums)
        return finish(placed, sums, chosen)

    outs = lax.switch(wide[0, 0], (finish, gather), placed, sums, chosen)
    return tuple(x.reshape(cap) for x in outs)


def solution(mesh):
    (axis,) = mesh.axis_names
    n = mesh.shape[axis]
    placed = (P(axis), P(axis), P(axis), P(axis), P(), P(), P())
    return jax.shard_map(
        functools.partial(shards, axis, n),
        mesh=mesh,
        in_specs=placed,
        out_specs=(P(axis), P(axis), P(axis)),
        check_vma=False,
    )
```

```python
import functools

import jax
import jax.numpy as jnp
from jax import lax
from jax.experimental import pallas as pl
from jax.experimental.pallas import tpu as pltpu
from jax.sharding import PartitionSpec as P

MARGIN = 4096
LANES = 128
BLOCK = MARGIN // LANES
HALF = 64
HALF_BITS = 6
LANE_BITS = 7
PAD = BLOCK + 8
EDGE = 2 * PAD + BLOCK
TILE = 256
REACH = 4
UPDATE, WEIGHT, MOMENT, SECOND = range(4)


BETA_ONE = 0.9
BETA_TWO = 0.999
CORR_ONE = 1.0 - 0.9**10
CORR_TWO = 1.0 - 0.999**10
DECAY = 0.01
LEARN = 0.1
EPSILON = 1e-06

MESH = pl.DeviceIdType.MESH
VMEM_LIMIT = 16 * 1024 * 1024


def lane_ids(rows=BLOCK):
    return lax.broadcasted_iota(jnp.int32, (rows, LANES), 1)


def flat_ids():
    return lax.broadcasted_iota(jnp.int32, (BLOCK, LANES), 0) * LANES + lane_ids()


def moved(first, second, lanes):
    picked = jnp.where(lane_ids(first.shape[0]) >= lanes, first, second)
    return pltpu.roll(picked, (LANES - lanes) & (LANES - 1), 1)


def inverse(second):
    spread = second * (CORR_ONE * CORR_ONE / CORR_TWO)
    return 1.0 / (spread * lax.rsqrt(spread) + CORR_ONE * EPSILON)


def fetched(tables, refs, sems):
    copies = [pltpu.make_async_copy(t, r, sems.at[i]) for i, (t, r) in enumerate(zip(tables, refs))]
    for copy in copies:
        copy.start()
    return copies


def step_kernel(
    axis, n, old_hbm, new_hbm, seg_hbm, w_hbm, m_hbm, v_hbm, g_hbm, placed, sums, chosen, wide,
    state, m_buf, v_buf, g_buf, member, part, tail, left_rim, right_rim,
    before, after, slots, old_ref, new_ref, seg_ref, sems, table_sems, send, receive, rim_send, rim_receive,
):
    rows = m_buf.shape[0]
    blocks = rows // BLOCK
    segs = seg_ref.shape[1]
    me = lax.axis_index(axis)
    right = lax.rem(me + 1, n)
    left = lax.rem(me + n - 1, n)
    tables = fetched((old_hbm, new_hbm, seg_hbm), (old_ref, new_ref, seg_ref), table_sems)
    weights = state.at[WEIGHT, pl.ds(PAD, rows)]
    loads = fetched((v_hbm, g_hbm, m_hbm, w_hbm), (v_buf, g_buf, m_buf, weights), sems)
    barrier = pltpu.get_barrier_semaphore()
    near = [k for k in range(-REACH, REACH + 1) if k and abs(k) < n]

    def inside(k):
        return (me + k >= 0) & (me + k < n)

    for k in near:

        @pl.when(inside(k))
        def greet(k=k):
            pl.semaphore_signal(barrier, inc=1, device_id=(me + k,), device_id_type=MESH)

    for copy in tables:
        copy.wait()
    low = old_ref[me]
    count = old_ref[me + 1] - low
    new_low = new_ref[me]
    new_count = new_ref[me + 1] - new_low
    shift = new_low - low
    phase = (-low) & (HALF - 1)
    spot = lane_ids(segs)
    line = lax.broadcasted_iota(jnp.int32, (segs, LANES), 0)
    square_line = lax.broadcasted_iota(jnp.int32, (segs, segs), 0)
    square_spot = lax.broadcasted_iota(jnp.int32, (segs, segs), 1)
    starts = (seg_ref[...] >> HALF_BITS).astype(jnp.float32)
    first = jnp.sum(jnp.where(square_spot == square_line, starts, 0.0), axis=1, keepdims=True)
    past = jnp.sum(jnp.where(square_spot == square_line + 1, starts, 0.0), axis=1, keepdims=True)
    past = jnp.where(square_line[:, :1] == segs - 1, 4.0 * n * rows, past)
    first = jnp.broadcast_to(first.astype(jnp.int32), (segs, LANES))
    past = jnp.broadcast_to(past.astype(jnp.int32), (segs, LANES))
    base = (low + phase) >> HALF_BITS
    first_half = first - base
    past_half = past - base
    padded = member.shape[1]
    for group in range(3):
        for tile in range(padded // LANES):
            half = 2 * (spot + tile * LANES) - 1 + group
            mask = (half >= first_half) & (half < past_half)
            member[group * segs : (group + 1) * segs, tile * LANES : (tile + 1) * LANES] = jnp.where(
                mask, 1.0, 0.0
            ).astype(jnp.bfloat16)

    flat = flat_ids()

    spans = [(slice(r0, r0 + BLOCK), slice(r0 + PAD, r0 + PAD + BLOCK)) for r0 in range(0, rows, BLOCK)]
    for copy in loads[:2]:
        copy.wait()
    for here, there in spans:
        gradient = g_buf[here, :].astype(jnp.float32)
        second = BETA_TWO * v_buf[here, :] + ((1.0 - BETA_TWO) * gradient) * gradient
        state[UPDATE, there, :] = inverse(second)
        state[SECOND, there, :] = second
    loads[2].wait()
    for here, there in spans:
        moment = BETA_ONE * m_buf[here, :] + (1.0 - BETA_ONE) * g_buf[here, :].astype(jnp.float32)
        state[UPDATE, there, :] = moment * state[UPDATE, there, :]
        state[MOMENT, there, :] = moment
    loads[3].wait()
    peers = jnp.minimum(me, REACH) + jnp.minimum(n - 1 - me, REACH)
    pl.semaphore_wait(barrier, peers)
    start_row = (count - MARGIN) >> LANE_BITS
    for a in range(3):
        tail[a] = state[a + 1, pl.ds(PAD + start_row, BLOCK + 8), :]
    ragged = pl.ds(0, BLOCK + 1)
    onward = pltpu.make_async_remote_copy(
        src_ref=tail.at[:, ragged],
        dst_ref=left_rim.at[:, ragged],
        send_sem=rim_send.at[0],
        recv_sem=rim_receive.at[0],
        device_id=(right,),
        device_id_type=MESH,
    )
    back = pltpu.make_async_remote_copy(
        src_ref=state.at[pl.ds(1, 3), pl.ds(PAD, BLOCK)],
        dst_ref=right_rim,
        send_sem=rim_send.at[1],
        recv_sem=rim_receive.at[1],
        device_id=(left,),
        device_id_type=MESH,
    )

    @pl.when(me < n - 1)
    def send_tail():
        onward.start()

    @pl.when(me > 0)
    def send_head():
        back.start()

    product = None
    for t0 in range(0, rows, TILE):
        t1 = min(t0 + TILE, rows)
        pieces = [[], [], [], []]
        for r0 in range(t0, t1, BLOCK):
            there = slice(r0 + PAD, r0 + PAD + BLOCK)
            weight = state[WEIGHT, there, :]
            update = state[UPDATE, there, :] + DECAY * weight
            state[UPDATE, there, :] = update
            for i, value in enumerate((weight, update)):
                square = value * value
                if r0 + 2 * BLOCK >= rows:
                    square = jnp.where(flat + r0 * LANES < count, square, 0.0)
                coarse = square.astype(jnp.bfloat16)
                pieces[i].append(coarse)
                pieces[i + 2].append((square - coarse.astype(jnp.float32)).astype(jnp.bfloat16))
        squares = jnp.concatenate([jnp.concatenate(p, axis=0) for p in pieces], axis=1)
        partial = jnp.dot(member[:, t0:t1], squares, preferred_element_type=jnp.float32)
        product = partial if product is None else product + partial
    product = product[:, : 2 * LANES] + product[:, 2 * LANES :]
    on_lane = (spot & (segs - 1)) == line
    for i in range(2):
        columns = slice(i * LANES, (i + 1) * LANES)
        mixed = jnp.where(
            spot < phase,
            product[0:segs, columns],
            jnp.where(
                spot < phase + HALF, product[segs : 2 * segs, columns], product[2 * segs : 3 * segs, columns]
            ),
        )
        column = jnp.sum(mixed, axis=1, keepdims=True)
        part[i : i + 1, :] = jnp.sum(jnp.where(on_lane, column, 0.0), axis=0, keepdims=True)

    def tell(k):
        return pltpu.make_async_remote_copy(
            src_ref=part,
            dst_ref=slots.at[k + REACH],
            send_sem=send,
            recv_sem=receive,
            device_id=(me + k,),
            device_id_type=MESH,
        )

    for k in near:

        @pl.when(inside(k))
        def send_sums(k=k):
            tell(k).start()

    sums[3:5, :] = part[...]

    top = shift >> LANE_BITS
    lanes = shift & (LANES - 1)

    def own(a, b):
        there = b * BLOCK + PAD + top
        return moved(state[a, pl.ds(there, BLOCK), :], state[a, pl.ds(there + 1, BLOCK), :], lanes)

    def inner(b, carry):
        here = pl.multiple_of(b * BLOCK, BLOCK)
        for a in range(4):
            placed[a, pl.ds(here, BLOCK), :] = own(a, b)
        return carry

    lax.fori_loop(1, blocks - 3, inner, 0, unroll=3)
    for a in range(4):
        before[a, BLOCK:EDGE, :] = state[a, PAD : PAD + EDGE - BLOCK, :]
    for b in range(blocks - 3, blocks):
        live = flat + b * MARGIN < new_count
        for a in range(4):
            placed[a, b * BLOCK : (b + 1) * BLOCK, :] = jnp.where(live, own(a, b), 0.0)

    new_phase = (-new_low) & (HALF - 1)
    new_base = (new_low + new_phase) >> HALF_BITS
    lows = jnp.sum(jnp.where(on_lane, first - new_base, 0), axis=0, keepdims=True)
    highs = jnp.sum(jnp.where(on_lane, past - new_base, 0), axis=0, keepdims=True)
    block_row = lax.broadcasted_iota(jnp.int32, (BLOCK, LANES), 0)
    lane_group = lane_ids() >> HALF_BITS

    def choose(b, carry):
        here = pl.multiple_of(b * BLOCK, BLOCK)
        for tile in range(2):
            half = 2 * (block_row + b * BLOCK) - 1 + 2 * tile + lane_group
            mask = (half >= lows) & (half < highs)
            chosen[pl.ds(here, BLOCK), tile * LANES : (tile + 1) * LANES] = jnp.where(mask, 1.0, 0.0).astype(
                jnp.bfloat16
            )
        return carry

    lax.fori_loop(0, blocks, choose, 0, unroll=2)
    sums[2:3, :] = jnp.full((1, LANES), new_phase, jnp.int32).astype(jnp.float32)

    length = jnp.where(line == segs - 1, old_ref[n] >> HALF_BITS, past) - first
    most = (REACH * (rows * LANES - 2 * MARGIN) - MARGIN) >> HALF_BITS
    wide[...] = jnp.max(jnp.where(length > most, 1, 0), axis=0, keepdims=True)

    @pl.when(me < n - 1)
    def end_right():
        onward.wait_send()
        back.wait_recv()

    @pl.when(me > 0)
    def end_left():
        back.wait_send()
        onward.wait_recv()

    left_start = low - old_ref[jnp.maximum(me - 1, 0)] - MARGIN
    left_lane = left_start & (LANES - 1)
    left_rows = [moved(left_rim[a, 0:BLOCK, :], left_rim[a, 1 : BLOCK + 1, :], left_lane) for a in range(3)]
    right_rows = [right_rim[a] for a in range(3)]
    for ref, there, rim in ((before, slice(0, BLOCK), left_rows), (after, slice(PAD, PAD + BLOCK), right_rows)):
        for a in range(3):
            ref[a + 1, there, :] = rim[a]
        ref[UPDATE, there, :] = rim[1] * inverse(rim[2]) + DECAY * rim[0]
    side = (shift - count) & (LANES - 1)
    for a in range(4):
        after[a, PAD - 8 : PAD + BLOCK, :] = moved(
            after[a, PAD - 8 : PAD + BLOCK, :], after[a, PAD - 7 : PAD + BLOCK + 1, :], side
        )
    for a in range(4):
        placed[a, 0:BLOCK, :] = moved(
            before[a, pl.ds(BLOCK + top, BLOCK), :], before[a, pl.ds(BLOCK + top + 1, BLOCK), :], lanes
        )

    for b in range(blocks - 3, blocks):
        offset = b * MARGIN + shift - count
        edge = jnp.clip(offset >> LANE_BITS, -PAD, PAD - 7) + PAD
        index = flat + b * MARGIN
        beyond = (index + shift >= count) & (index < new_count)
        here = slice(b * BLOCK, (b + 1) * BLOCK)
        for a in range(4):
            placed[a, here, :] = jnp.where(beyond, after[a, pl.ds(edge, BLOCK), :], placed[a, here, :])

    def settle(semaphore):
        for c in sorted({min(i, REACH) + min(n - 1 - i, REACH) for i in range(n)}):

            @pl.when(peers == c)
            def end(c=c):
                some = slots.at[pl.ds(0, c)]
                pltpu.make_async_copy(some, some, semaphore).wait()

    settle(send)
    settle(receive)
    total = part[...]
    for k in near:
        total = total + jnp.where(inside(-k), slots[k + REACH], 0.0)
    sums[0:2, :] = total


def everyone_kernel(axis, n, near_sums, sums, part, slots, send, receive):
    me = lax.axis_index(axis)
    barrier = pltpu.get_barrier_semaphore()

    def greet(k, carry):
        pl.semaphore_signal(barrier, inc=1, device_id=(lax.rem(me + k, n),), device_id_type=MESH)
        return carry

    lax.fori_loop(1, n, greet, 0)
    part[...] = near_sums[3:5, :]
    sums[2:5, :] = near_sums[2:5, :]
    pl.semaphore_wait(barrier, n - 1)

    def tell(k, carry):
        pltpu.make_async_remote_copy(
            src_ref=part,
            dst_ref=slots.at[me],
            send_sem=send,
            recv_sem=receive,
            device_id=(lax.rem(me + k, n),),
            device_id_type=MESH,
        ).start()
        return carry

    lax.fori_loop(1, n, tell, 0)
    pltpu.make_async_copy(part, slots.at[me], receive).start()
    pltpu.make_async_copy(slots, slots, receive).wait()
    sums[0:2, :] = jnp.sum(slots[...], axis=0)
    others = slots.at[pl.ds(0, n - 1)]
    pltpu.make_async_copy(others, others, send).wait()


def apply_kernel(segs, placed, sums, chosen, w_out, m_out, v_out, w_buf, sems):
    m_copy = pltpu.make_async_copy(placed.at[MOMENT], m_out, sems.at[0])
    v_copy = pltpu.make_async_copy(placed.at[SECOND], v_out, sems.at[1])
    m_copy.start()
    v_copy.start()
    rows = w_buf.shape[0]
    total = sums[0:1, :]
    other = sums[1:2, :]
    phase = sums[2:3, :]
    rate = LEARN * (jnp.sqrt(total) / (jnp.sqrt(other) + EPSILON))
    place = lax.broadcasted_iota(jnp.int32, (LANES, LANES), 0).astype(jnp.float32)
    lower = lane_ids(LANES) < segs
    early = place < phase
    late = place >= phase + HALF
    rates = jnp.concatenate(
        [
            jnp.where((lower & early) | ~(lower | early | late), rate, 0.0),
            jnp.where(lower & late, rate, 0.0),
        ],
        axis=1,
    )
    coarse = rates.astype(jnp.bfloat16)
    fine = (rates - coarse.astype(jnp.float32)).astype(jnp.bfloat16)
    table = jnp.concatenate([coarse, fine], axis=0)
    step = 256
    copies = []
    for c, r0 in enumerate(range(0, rows, step)):
        size = min(step, rows - r0)
        product = lax.dot_general(
            chosen[r0 : r0 + size, :], table, (((1,), (1,)), ((), ())), preferred_element_type=jnp.float32
        )
        factor = product[:, :LANES] + product[:, LANES:]
        w_buf[r0 : r0 + size, :] = placed[WEIGHT, r0 : r0 + size, :] - factor * placed[UPDATE, r0 : r0 + size, :]
        window = pl.ds(r0, size)
        copy = pltpu.make_async_copy(w_buf.at[window], w_out.at[window], sems.at[2 + c])
        copy.start()
        copies.append(copy)
    for copy in (m_copy, v_copy, *copies):
        copy.wait()


def spec(space):
    return pl.BlockSpec(memory_space=space)


def shards(axis, n, params, first_moment, second_moment, grads, old_bounds, new_bounds, seg_start):
    cap = params.shape[0]
    rows = cap // LANES
    f32 = jnp.float32
    flat = [x.reshape(rows, LANES) for x in (params, first_moment, second_moment, grads)]
    segs = seg_start.shape[0]
    tables = (old_bounds, new_bounds, seg_start.reshape(1, segs))
    old_bounds, new_bounds, starts_row, *flat = (
        pltpu.with_memory_space_constraint(x, pltpu.HBM) for x in (*tables, *flat)
    )
    padded = -(-rows // LANES) * LANES
    vmem, hbm = spec(pltpu.VMEM), spec(pltpu.HBM)
    bounds = pltpu.SMEM(old_bounds.shape, jnp.int32)
    starts = pltpu.VMEM((1, segs), jnp.int32)
    rim = pltpu.VMEM((3, BLOCK, LANES), f32)
    ragged = pltpu.VMEM((3, BLOCK + 8, LANES), f32)
    dma = pltpu.SemaphoreType.DMA
    placed, sums, chosen, wide = pl.pallas_call(
        functools.partial(step_kernel, axis, n),
        name="step",
        out_shape=(
            jax.ShapeDtypeStruct((4, rows, LANES), f32),
            jax.ShapeDtypeStruct((5, LANES), f32),
            jax.ShapeDtypeStruct((rows, 2 * LANES), jnp.bfloat16),
            jax.ShapeDtypeStruct((1, LANES), jnp.int32),
        ),
        in_specs=[hbm] * 7,
        out_specs=(vmem, vmem, vmem, vmem),
        scratch_shapes=[
            pltpu.VMEM((4, rows + 2 * PAD, LANES), f32),
            pltpu.VMEM((rows, LANES), f32),
            pltpu.VMEM((rows, LANES), f32),
            pltpu.VMEM((rows, LANES), grads.dtype),
            pltpu.VMEM((3 * segs, padded), jnp.bfloat16),
            pltpu.VMEM((2, LANES), f32),
            ragged,
            ragged,
            rim,
            pltpu.VMEM((4, EDGE, LANES), f32),
            pltpu.VMEM((4, EDGE, LANES), f32),
            pltpu.VMEM((2 * REACH + 1, 2, LANES), f32),
            bounds,
            bounds,
            starts,
            dma((4,)),
            dma((3,)),
            dma,
            dma,
            dma((2,)),
            dma((2,)),
        ],
        compiler_params=pltpu.CompilerParams(
            collective_id=0, has_side_effects=True, vmem_limit_bytes=VMEM_LIMIT
        ),
    )(old_bounds, new_bounds, starts_row, *flat)
    whole = jax.ShapeDtypeStruct((rows, LANES), f32)
    def finish(placed, sums, chosen):
        return pl.pallas_call(
            functools.partial(apply_kernel, segs),
            name="apply",
            out_shape=(whole,) * 3,
            in_specs=[vmem] * 3,
            out_specs=(hbm,) * 3,
            scratch_shapes=[pltpu.VMEM((rows, LANES), f32), dma((2 + -(-rows // 256),))],
            compiler_params=pltpu.CompilerParams(vmem_limit_bytes=VMEM_LIMIT),
        )(placed, sums, chosen)

    def gather(placed, sums, chosen):
        sums = pl.pallas_call(
            functools.partial(everyone_kernel, axis, n),
            name="everyone",
            out_shape=jax.ShapeDtypeStruct((5, LANES), f32),
            in_specs=[vmem],
            out_specs=vmem,
            scratch_shapes=[pltpu.VMEM((2, LANES), f32), pltpu.VMEM((n, 2, LANES), f32), dma, dma],
            compiler_params=pltpu.CompilerParams(
                collective_id=1, has_side_effects=True, vmem_limit_bytes=VMEM_LIMIT
            ),
        )(sums)
        return finish(placed, sums, chosen)

    outs = lax.switch(wide[0, 0], (finish, gather), placed, sums, chosen)
    return tuple(x.reshape(cap) for x in outs)


def solution(mesh):
    (axis,) = mesh.axis_names
    n = mesh.shape[axis]
    placed = (P(axis), P(axis), P(axis), P(axis), P(), P(), P())
    return jax.shard_map(
        functools.partial(shards, axis, n),
        mesh=mesh,
        in_specs=placed,
        out_specs=(P(axis), P(axis), P(axis)),
        check_vma=False,
    )
```

```python
import functools

import jax
import jax.numpy as jnp
from jax import lax
from jax.experimental import pallas as pl
from jax.experimental.pallas import tpu as pltpu
from jax.sharding import PartitionSpec as P

MARGIN = 4096
LANES = 128
BLOCK = MARGIN // LANES
HALF = 64
HALF_BITS = 6
LANE_BITS = 7
PAD = BLOCK + 8
EDGE = 2 * PAD + BLOCK
TILE = 1024
REACH = 4
UPDATE, WEIGHT, MOMENT, SECOND = range(4)


BETA_ONE = 0.9
BETA_TWO = 0.999
CORR_ONE = 1.0 - 0.9**10
CORR_TWO = 1.0 - 0.999**10
DECAY = 0.01
LEARN = 0.1
EPSILON = 1e-06

MESH = pl.DeviceIdType.MESH
VMEM_LIMIT = 16 * 1024 * 1024


def lane_ids(rows=BLOCK):
    return lax.broadcasted_iota(jnp.int32, (rows, LANES), 1)


def flat_ids():
    return lax.broadcasted_iota(jnp.int32, (BLOCK, LANES), 0) * LANES + lane_ids()


def moved(first, second, lanes):
    picked = jnp.where(lane_ids(first.shape[0]) >= lanes, first, second)
    return pltpu.roll(picked, (LANES - lanes) & (LANES - 1), 1)


def inverse(second):
    spread = second * (CORR_ONE * CORR_ONE / CORR_TWO)
    return 1.0 / (spread * lax.rsqrt(spread) + CORR_ONE * EPSILON)


def fetched(tables, refs, sems):
    copies = [pltpu.make_async_copy(t, r, sems.at[i]) for i, (t, r) in enumerate(zip(tables, refs))]
    for copy in copies:
        copy.start()
    return copies


def step_kernel(
    axis, n, old_hbm, new_hbm, seg_hbm, w_hbm, m_hbm, v_hbm, g_hbm, placed, sums, chosen, wide,
    state, m_buf, v_buf, g_buf, member, part, tail, left_rim, right_rim,
    before, after, slots, old_ref, new_ref, seg_ref, sems, send, receive, rim_send, rim_receive,
):
    rows = m_buf.shape[0]
    blocks = rows // BLOCK
    segs = seg_ref.shape[1]
    me = lax.axis_index(axis)
    right = lax.rem(me + 1, n)
    left = lax.rem(me + n - 1, n)
    tables = [
        pltpu.make_async_copy(old_hbm, old_ref, rim_send.at[0]),
        pltpu.make_async_copy(new_hbm, new_ref, rim_send.at[1]),
        pltpu.make_async_copy(seg_hbm, seg_ref, send),
    ]
    for copy in tables:
        copy.start()
    weights = state.at[WEIGHT, pl.ds(PAD, rows)]
    loads = fetched((v_hbm, g_hbm, m_hbm, w_hbm), (v_buf, g_buf, m_buf, weights), sems)
    barrier = pltpu.get_barrier_semaphore()
    near = [k for k in range(-REACH, REACH + 1) if k and abs(k) < n]

    def inside(k):
        return (me + k >= 0) & (me + k < n)

    for k in near:

        @pl.when(inside(k))
        def greet(k=k):
            pl.semaphore_signal(barrier, inc=1, device_id=(me + k,), device_id_type=MESH)

    for copy in tables:
        copy.wait()
    low = old_ref[me]
    count = old_ref[me + 1] - low
    new_low = new_ref[me]
    new_count = new_ref[me + 1] - new_low
    shift = new_low - low
    phase = (-low) & (HALF - 1)
    spot = lane_ids(segs)
    line = lax.broadcasted_iota(jnp.int32, (segs, LANES), 0)
    square_line = lax.broadcasted_iota(jnp.int32, (segs, segs), 0)
    square_spot = lax.broadcasted_iota(jnp.int32, (segs, segs), 1)
    starts = (seg_ref[...] >> HALF_BITS).astype(jnp.float32)
    first = jnp.sum(jnp.where(square_spot == square_line, starts, 0.0), axis=1, keepdims=True)
    past = jnp.sum(jnp.where(square_spot == square_line + 1, starts, 0.0), axis=1, keepdims=True)
    past = jnp.where(square_line[:, :1] == segs - 1, 4.0 * n * rows, past)
    first = jnp.broadcast_to(first.astype(jnp.int32), (segs, LANES))
    past = jnp.broadcast_to(past.astype(jnp.int32), (segs, LANES))
    base = (low + phase) >> HALF_BITS
    first_half = first - base
    past_half = past - base
    padded = member.shape[1]
    for group in range(3):
        for tile in range(padded // LANES):
            half = 2 * (spot + tile * LANES) - 1 + group
            mask = (half >= first_half) & (half < past_half)
            member[group * segs : (group + 1) * segs, tile * LANES : (tile + 1) * LANES] = jnp.where(
                mask, 1.0, 0.0
            ).astype(jnp.bfloat16)

    flat = flat_ids()

    spans = [(slice(r0, r0 + BLOCK), slice(r0 + PAD, r0 + PAD + BLOCK)) for r0 in range(0, rows, BLOCK)]
    for copy in loads[:2]:
        copy.wait()
    for here, there in spans:
        gradient = g_buf[here, :].astype(jnp.float32)
        second = BETA_TWO * v_buf[here, :] + ((1.0 - BETA_TWO) * gradient) * gradient
        state[UPDATE, there, :] = inverse(second)
        state[SECOND, there, :] = second
    loads[2].wait()
    for here, there in spans:
        moment = BETA_ONE * m_buf[here, :] + (1.0 - BETA_ONE) * g_buf[here, :].astype(jnp.float32)
        state[UPDATE, there, :] = moment * state[UPDATE, there, :]
        state[MOMENT, there, :] = moment
    loads[3].wait()
    peers = jnp.minimum(me, REACH) + jnp.minimum(n - 1 - me, REACH)
    pl.semaphore_wait(barrier, peers)
    start_row = (count - MARGIN) >> LANE_BITS
    for a in range(3):
        tail[a] = state[a + 1, pl.ds(PAD + start_row, BLOCK + 8), :]
    ragged = pl.ds(0, BLOCK + 1)
    onward = pltpu.make_async_remote_copy(
        src_ref=tail.at[:, ragged],
        dst_ref=left_rim.at[:, ragged],
        send_sem=rim_send.at[0],
        recv_sem=rim_receive.at[0],
        device_id=(right,),
        device_id_type=MESH,
    )
    back = pltpu.make_async_remote_copy(
        src_ref=state.at[pl.ds(1, 3), pl.ds(PAD, BLOCK)],
        dst_ref=right_rim,
        send_sem=rim_send.at[1],
        recv_sem=rim_receive.at[1],
        device_id=(left,),
        device_id_type=MESH,
    )

    @pl.when(me < n - 1)
    def send_tail():
        onward.start()

    @pl.when(me > 0)
    def send_head():
        back.start()

    product = None
    for t0 in range(0, rows, TILE):
        t1 = min(t0 + TILE, rows)
        pieces = [[], [], [], []]
        for r0 in range(t0, t1, BLOCK):
            there = slice(r0 + PAD, r0 + PAD + BLOCK)
            weight = state[WEIGHT, there, :]
            update = state[UPDATE, there, :] + DECAY * weight
            state[UPDATE, there, :] = update
            for i, value in enumerate((weight, update)):
                square = value * value
                if r0 + 2 * BLOCK >= rows:
                    square = jnp.where(flat + r0 * LANES < count, square, 0.0)
                coarse = square.astype(jnp.bfloat16)
                pieces[i].append(coarse)
                pieces[i + 2].append((square - coarse.astype(jnp.float32)).astype(jnp.bfloat16))
        squares = jnp.concatenate([jnp.concatenate(p, axis=0) for p in pieces], axis=1)
        partial = jnp.dot(member[:, t0:t1], squares, preferred_element_type=jnp.float32)
        product = partial if product is None else product + partial
    product = product[:, : 2 * LANES] + product[:, 2 * LANES :]
    on_lane = (spot & (segs - 1)) == line
    for i in range(2):
        columns = slice(i * LANES, (i + 1) * LANES)
        mixed = jnp.where(
            spot < phase,
            product[0:segs, columns],
            jnp.where(
                spot < phase + HALF, product[segs : 2 * segs, columns], product[2 * segs : 3 * segs, columns]
            ),
        )
        column = jnp.sum(mixed, axis=1, keepdims=True)
        part[i : i + 1, :] = jnp.sum(jnp.where(on_lane, column, 0.0), axis=0, keepdims=True)

    def tell(k):
        return pltpu.make_async_remote_copy(
            src_ref=part,
            dst_ref=slots.at[k + REACH],
            send_sem=send,
            recv_sem=receive,
            device_id=(me + k,),
            device_id_type=MESH,
        )

    for k in near:

        @pl.when(inside(k))
        def send_sums(k=k):
            tell(k).start()

    sums[3:5, :] = part[...]

    top = shift >> LANE_BITS
    lanes = shift & (LANES - 1)

    def own(a, b):
        there = b * BLOCK + PAD + top
        return moved(state[a, pl.ds(there, BLOCK), :], state[a, pl.ds(there + 1, BLOCK), :], lanes)

    def inner(b, carry):
        here = pl.multiple_of(b * BLOCK, BLOCK)
        for a in range(4):
            placed[a, pl.ds(here, BLOCK), :] = own(a, b)
        return carry

    lax.fori_loop(1, blocks - 3, inner, 0, unroll=3)
    for a in range(4):
        before[a, BLOCK:EDGE, :] = state[a, PAD : PAD + EDGE - BLOCK, :]
    for b in range(blocks - 3, blocks):
        live = flat + b * MARGIN < new_count
        for a in range(4):
            placed[a, b * BLOCK : (b + 1) * BLOCK, :] = jnp.where(live, own(a, b), 0.0)

    new_phase = (-new_low) & (HALF - 1)
    new_base = (new_low + new_phase) >> HALF_BITS
    lows = jnp.sum(jnp.where(on_lane, first - new_base, 0), axis=0, keepdims=True)
    highs = jnp.sum(jnp.where(on_lane, past - new_base, 0), axis=0, keepdims=True)
    block_row = lax.broadcasted_iota(jnp.int32, (BLOCK, LANES), 0)
    lane_group = lane_ids() >> HALF_BITS

    def choose(b, carry):
        here = pl.multiple_of(b * BLOCK, BLOCK)
        for tile in range(2):
            half = 2 * (block_row + b * BLOCK) - 1 + 2 * tile + lane_group
            mask = (half >= lows) & (half < highs)
            chosen[pl.ds(here, BLOCK), tile * LANES : (tile + 1) * LANES] = jnp.where(mask, 1.0, 0.0).astype(
                jnp.bfloat16
            )
        return carry

    lax.fori_loop(0, blocks, choose, 0, unroll=2)
    sums[2:3, :] = jnp.full((1, LANES), new_phase, jnp.int32).astype(jnp.float32)

    length = jnp.where(line == segs - 1, old_ref[n] >> HALF_BITS, past) - first
    most = (REACH * (rows * LANES - 2 * MARGIN) - MARGIN) >> HALF_BITS
    wide[...] = jnp.max(jnp.where(length > most, 1, 0), axis=0, keepdims=True)

    @pl.when(me < n - 1)
    def end_right():
        onward.wait_send()
        back.wait_recv()

    @pl.when(me > 0)
    def end_left():
        back.wait_send()
        onward.wait_recv()

    left_start = low - old_ref[jnp.maximum(me - 1, 0)] - MARGIN
    left_lane = left_start & (LANES - 1)
    left_rows = [moved(left_rim[a, 0:BLOCK, :], left_rim[a, 1 : BLOCK + 1, :], left_lane) for a in range(3)]
    right_rows = [right_rim[a] for a in range(3)]
    for ref, there, rim in ((before, slice(0, BLOCK), left_rows), (after, slice(PAD, PAD + BLOCK), right_rows)):
        for a in range(3):
            ref[a + 1, there, :] = rim[a]
        ref[UPDATE, there, :] = rim[1] * inverse(rim[2]) + DECAY * rim[0]
    side = (shift - count) & (LANES - 1)
    for a in range(4):
        after[a, PAD - 8 : PAD + BLOCK, :] = moved(
            after[a, PAD - 8 : PAD + BLOCK, :], after[a, PAD - 7 : PAD + BLOCK + 1, :], side
        )
    for a in range(4):
        placed[a, 0:BLOCK, :] = moved(
            before[a, pl.ds(BLOCK + top, BLOCK), :], before[a, pl.ds(BLOCK + top + 1, BLOCK), :], lanes
        )

    for b in range(blocks - 3, blocks):
        offset = b * MARGIN + shift - count
        edge = jnp.clip(offset >> LANE_BITS, -PAD, PAD - 7) + PAD
        index = flat + b * MARGIN
        beyond = (index + shift >= count) & (index < new_count)
        here = slice(b * BLOCK, (b + 1) * BLOCK)
        for a in range(4):
            placed[a, here, :] = jnp.where(beyond, after[a, pl.ds(edge, BLOCK), :], placed[a, here, :])

    def settle(semaphore):
        for c in sorted({min(i, REACH) + min(n - 1 - i, REACH) for i in range(n)}):

            @pl.when(peers == c)
            def end(c=c):
                some = slots.at[pl.ds(0, c)]
                pltpu.make_async_copy(some, some, semaphore).wait()

    settle(send)
    settle(receive)
    total = part[...]
    for k in near:
        total = total + jnp.where(inside(-k), slots[k + REACH], 0.0)
    sums[0:2, :] = total


def everyone_kernel(axis, n, near_sums, sums, part, slots, send, receive):
    me = lax.axis_index(axis)
    barrier = pltpu.get_barrier_semaphore()

    def greet(k, carry):
        pl.semaphore_signal(barrier, inc=1, device_id=(lax.rem(me + k, n),), device_id_type=MESH)
        return carry

    lax.fori_loop(1, n, greet, 0)
    part[...] = near_sums[3:5, :]
    sums[2:5, :] = near_sums[2:5, :]
    pl.semaphore_wait(barrier, n - 1)

    def tell(k, carry):
        pltpu.make_async_remote_copy(
            src_ref=part,
            dst_ref=slots.at[me],
            send_sem=send,
            recv_sem=receive,
            device_id=(lax.rem(me + k, n),),
            device_id_type=MESH,
        ).start()
        return carry

    lax.fori_loop(1, n, tell, 0)
    pltpu.make_async_copy(part, slots.at[me], receive).start()
    pltpu.make_async_copy(slots, slots, receive).wait()
    sums[0:2, :] = jnp.sum(slots[...], axis=0)
    others = slots.at[pl.ds(0, n - 1)]
    pltpu.make_async_copy(others, others, send).wait()


def apply_kernel(segs, placed, sums, chosen, w_out, m_out, v_out, w_buf, sems):
    m_copy = pltpu.make_async_copy(placed.at[MOMENT], m_out, sems.at[0])
    v_copy = pltpu.make_async_copy(placed.at[SECOND], v_out, sems.at[1])
    m_copy.start()
    v_copy.start()
    rows = w_buf.shape[0]
    total = sums[0:1, :]
    other = sums[1:2, :]
    phase = sums[2:3, :]
    rate = LEARN * (jnp.sqrt(total) / (jnp.sqrt(other) + EPSILON))
    place = lax.broadcasted_iota(jnp.int32, (LANES, LANES), 0).astype(jnp.float32)
    lower = lane_ids(LANES) < segs
    early = place < phase
    late = place >= phase + HALF
    rates = jnp.concatenate(
        [
            jnp.where((lower & early) | ~(lower | early | late), rate, 0.0),
            jnp.where(lower & late, rate, 0.0),
        ],
        axis=1,
    )
    coarse = rates.astype(jnp.bfloat16)
    fine = (rates - coarse.astype(jnp.float32)).astype(jnp.bfloat16)
    table = jnp.concatenate([coarse, fine], axis=0)
    step = 256
    copies = []
    for c, r0 in enumerate(range(0, rows, step)):
        size = min(step, rows - r0)
        product = lax.dot_general(
            chosen[r0 : r0 + size, :], table, (((1,), (1,)), ((), ())), preferred_element_type=jnp.float32
        )
        factor = product[:, :LANES] + product[:, LANES:]
        w_buf[r0 : r0 + size, :] = placed[WEIGHT, r0 : r0 + size, :] - factor * placed[UPDATE, r0 : r0 + size, :]
        window = pl.ds(r0, size)
        copy = pltpu.make_async_copy(w_buf.at[window], w_out.at[window], sems.at[2 + c])
        copy.start()
        copies.append(copy)
    for copy in (m_copy, v_copy, *copies):
        copy.wait()


def spec(space):
    return pl.BlockSpec(memory_space=space)


def shards(axis, n, params, first_moment, second_moment, grads, old_bounds, new_bounds, seg_start):
    cap = params.shape[0]
    rows = cap // LANES
    f32 = jnp.float32
    flat = [x.reshape(rows, LANES) for x in (params, first_moment, second_moment, grads)]
    segs = seg_start.shape[0]
    tables = (old_bounds, new_bounds, seg_start.reshape(1, segs))
    old_bounds, new_bounds, starts_row, *flat = (
        pltpu.with_memory_space_constraint(x, pltpu.HBM) for x in (*tables, *flat)
    )
    padded = -(-rows // LANES) * LANES
    vmem, hbm = spec(pltpu.VMEM), spec(pltpu.HBM)
    bounds = pltpu.SMEM(old_bounds.shape, jnp.int32)
    starts = pltpu.VMEM((1, segs), jnp.int32)
    rim = pltpu.VMEM((3, BLOCK, LANES), f32)
    ragged = pltpu.VMEM((3, BLOCK + 8, LANES), f32)
    dma = pltpu.SemaphoreType.DMA
    placed, sums, chosen, wide = pl.pallas_call(
        functools.partial(step_kernel, axis, n),
        name="step",
        out_shape=(
            jax.ShapeDtypeStruct((4, rows, LANES), f32),
            jax.ShapeDtypeStruct((5, LANES), f32),
            jax.ShapeDtypeStruct((rows, 2 * LANES), jnp.bfloat16),
            jax.ShapeDtypeStruct((1, LANES), jnp.int32),
        ),
        in_specs=[hbm] * 7,
        out_specs=(vmem, vmem, vmem, vmem),
        scratch_shapes=[
            pltpu.VMEM((4, rows + 2 * PAD, LANES), f32),
            pltpu.VMEM((rows, LANES), f32),
            pltpu.VMEM((rows, LANES), f32),
            pltpu.VMEM((rows, LANES), grads.dtype),
            pltpu.VMEM((3 * segs, padded), jnp.bfloat16),
            pltpu.VMEM((2, LANES), f32),
            ragged,
            ragged,
            rim,
            pltpu.VMEM((4, EDGE, LANES), f32),
            pltpu.VMEM((4, EDGE, LANES), f32),
            pltpu.VMEM((2 * REACH + 1, 2, LANES), f32),
            bounds,
            bounds,
            starts,
            dma((4,)),
            dma,
            dma,
            dma((2,)),
            dma((2,)),
        ],
        compiler_params=pltpu.CompilerParams(
            collective_id=0, has_side_effects=True, vmem_limit_bytes=VMEM_LIMIT
        ),
    )(old_bounds, new_bounds, starts_row, *flat)
    whole = jax.ShapeDtypeStruct((rows, LANES), f32)
    def finish(placed, sums, chosen):
        return pl.pallas_call(
            functools.partial(apply_kernel, segs),
            name="apply",
            out_shape=(whole,) * 3,
            in_specs=[vmem] * 3,
            out_specs=(hbm,) * 3,
            scratch_shapes=[pltpu.VMEM((rows, LANES), f32), dma((2 + -(-rows // 256),))],
            compiler_params=pltpu.CompilerParams(vmem_limit_bytes=VMEM_LIMIT),
        )(placed, sums, chosen)

    def gather(placed, sums, chosen):
        sums = pl.pallas_call(
            functools.partial(everyone_kernel, axis, n),
            name="everyone",
            out_shape=jax.ShapeDtypeStruct((5, LANES), f32),
            in_specs=[vmem],
            out_specs=vmem,
            scratch_shapes=[pltpu.VMEM((2, LANES), f32), pltpu.VMEM((n, 2, LANES), f32), dma, dma],
            compiler_params=pltpu.CompilerParams(
                collective_id=1, has_side_effects=True, vmem_limit_bytes=VMEM_LIMIT
            ),
        )(sums)
        return finish(placed, sums, chosen)

    outs = lax.switch(wide[0, 0], (finish, gather), placed, sums, chosen)
    return tuple(x.reshape(cap) for x in outs)


def solution(mesh):
    (axis,) = mesh.axis_names
    n = mesh.shape[axis]
    placed = (P(axis), P(axis), P(axis), P(axis), P(), P(), P())
    return jax.shard_map(
        functools.partial(shards, axis, n),
        mesh=mesh,
        in_specs=placed,
        out_specs=(P(axis), P(axis), P(axis)),
        check_vma=False,
    )
```
